256 devices in a mesh: sub: 8 (over y_lo, x), col: 16 (over z, core), grp: 2 (over y_hi).
Axes of the slice: x: 4, y: 4 (y_hi: 2, y_lo: 2; y = y_hi * 2 + y_lo), z: 8, core: 2. Of those that a mesh axis runs over, the one named last changes fastest.
Arguments:
- first_rhs: float32 [8, 640, 2048], P('sub', None, 'col'), may hold values from -6 to 6
- innovations: float32 [8, 1024, 640], P('sub', 'col'), may hold values from -6 to 6
- start_mult: float32 [8, 640, 2048], P('sub', None, 'col'), may hold values from -4 to 4
- trajectory: bfloat16 [8, 640, 2048], P('sub', None, 'col'), may hold values from -6 to 6
- weight_in: float32 [4096, 640], P('grp'), may hold values from -0.25 to 0.25
- weight_out: float32 [640, 4096], P(None, 'grp'), may hold values from -0.09375 to 0.09375
- vertical_modes: float32 [640, 640], P('grp'), may hold values from -0.25 to 0.25
- length_scale: float32 [640], replicated, may hold values from 2 to 16
- band_limit: int32 [640], replicated, may hold values from 1 to 128
- obs_col: int32 [8, 1024], P('sub', 'col'), may hold values from 0 to 2047, as said below
- obs_count: int32 [8, 16], P('sub', 'col'), may hold values from 1 to 64
- obs_var: float32 [8, 1024], P('sub', 'col'), may hold values from 0.25 to 4
Outputs:
- multiplier: float32 [8, 640, 2048], P('sub', None, 'col')
- obs_multiplier: float32 [8, 1024, 640], P('sub', 'col')
- increment: float32 [8, 640, 2048], P('sub', None, 'col')
The draws below stay inside these ranges and needn't reach their ends.
Inputs may be any that keep to these rules, and one draw needn't show every extreme that they name: `obs_col`: slot j of a subwindow observes a column of shard j // 64: a column from (j // 64) * 128 to (j // 64 + 1) * 128 - 1.
All inputs are finite; a program needn't handle non-finite values.
Results may differ from the reference program's by a relative error of at most 0.0003.
Values sent between devices are 32-bit elements; how exact they have to be, the bound alone decides.
A program may use at most 128 MiB of HBM per device.

```python
import math
import jax
import jax.numpy as jnp
from jax import lax

D = 640
HID = 4096
COLS_DEV = 128
OBS_DEV = 64
KW = 128
ITERS = 2
SUBS = 8
SHARDS = 16
COLS = 2048
SLOTS = 1024


def draw_obs_col(key, part):
    offsets = jax.random.randint(key, (SUBS, SLOTS), 0, COLS_DEV)
    base = jnp.arange(SLOTS, dtype=jnp.int32) // OBS_DEV * COLS_DEV
    return (offsets + base[None, :]).astype(jnp.int32)


def touch_ends(result, key, smallest, top_value):
    index_at = [jax.random.randint(jax.random.fold_in(key, axis), (), 0, length) for axis, length in enumerate(result.shape)]
    longest = result.shape.index(max(result.shape))
    beside = index_at[:longest] + [(index_at[longest] + 1) % result.shape[longest]] + index_at[longest + 1:]
    return result.at[tuple(index_at)].set(smallest).at[tuple(beside)].set(top_value)


def levels(stream_key, shape, cuts, smallest, top_value):
    gain = 1.0
    for dim, blocks in cuts:
        steps = jax.random.uniform(jax.random.fold_in(jax.random.fold_in(stream_key, 6), dim), (blocks,), jnp.float32, smallest / len(cuts), top_value / len(cuts))
        gain = gain * jnp.repeat(jnp.exp(steps), shape[dim] // blocks).reshape((-1,) + (1,) * (len(shape) - 1 - dim))
    return gain


def scatter_about(stream_key, dims, scale, bound, cuts=(), held_as=jnp.bfloat16):
    loudness = levels(stream_key, dims, cuts, -0.22, 0.18) if cuts else 1.0
    result = jax.random.normal(stream_key, dims, jnp.float32) * scale * loudness
    return jnp.minimum(jnp.maximum(result, -bound), bound).astype(held_as)


def setup_inputs(seed: int = 0) -> dict:
    arg_keys = jax.random.split(jax.random.key(seed), 13)
    first_rhs = scatter_about(arg_keys[0], (SUBS, D, COLS), 1.0, 6.0, ((0, 8), (2, 16)), jnp.float32)
    innovations = scatter_about(arg_keys[1], (SUBS, SLOTS, D), 1.0, 6.0, ((0, 8), (1, 16)), jnp.float32)
    start_mult = scatter_about(arg_keys[2], (SUBS, D, COLS), 0.5, 4.0, ((0, 8), (2, 16)), jnp.float32)
    trajectory = scatter_about(arg_keys[3], (SUBS, D, COLS), 1.0, 6.0, ((0, 8), (2, 16)))
    weight_in = scatter_about(arg_keys[4], (HID, D), D ** -0.5, 0.25, ((0, 2),), jnp.float32)
    weight_out = scatter_about(arg_keys[5], (D, HID), HID ** -0.5, 0.09375, ((1, 2),), jnp.float32)
    vertical_modes = scatter_about(arg_keys[6], (D, D), D ** -0.5, 0.25, ((0, 2),), jnp.float32)
    length_scale = jnp.clip(jnp.exp(jax.random.uniform(arg_keys[7], (D,), jnp.float32, math.log(2.0), math.log(16.0))), 2.0, 16.0)
    band_limit = touch_ends(jax.random.randint(arg_keys[8], (D,), 1, KW + 1), jax.random.fold_in(arg_keys[8], 1), 1, KW).astype(jnp.int32)
    obs_col = draw_obs_col(jax.random.fold_in(arg_keys[12], 71), 0)
    obs_count = touch_ends(jax.random.randint(arg_keys[10], (SUBS, SHARDS), 1, OBS_DEV + 1), jax.random.fold_in(arg_keys[10], 1), 1, OBS_DEV).astype(jnp.int32)
    obs_var = jnp.clip(jnp.exp(math.log(4.0) - 2.7725887 * jax.random.uniform(arg_keys[11], (SUBS, SLOTS), jnp.float32) ** levels(arg_keys[11], (SUBS, SLOTS), ((0, 8), (1, 16)), -0.2, 0.2)), 0.25, 4.0)
    return dict(first_rhs=first_rhs, innovations=innovations, start_mult=start_mult, trajectory=trajectory, weight_in=weight_in, weight_out=weight_out, vertical_modes=vertical_modes, length_scale=length_scale, band_limit=band_limit, obs_col=obs_col, obs_count=obs_count, obs_var=obs_var)


HIGH = lax.Precision.HIGHEST


def spectral_table(columns, count, total):
    waves = jnp.arange(count, dtype=jnp.int32)
    phase = (columns[:, None] * waves[None, :]) % total
    angle = (2.0 * math.pi / total) * phase.astype(jnp.float32)
    return jnp.concatenate([jnp.cos(angle), jnp.sin(angle)], axis=1)


def spectrum(scales, limits, total, count):
    waves = jnp.arange(count, dtype=jnp.int32)
    wavef = waves.astype(jnp.float32)
    decay = jnp.exp(-0.5 * (2.0 * math.pi * wavef[None, :] * scales[:, None] / total) ** 2)
    factor = jnp.where(waves == 0, 1.0, 2.0).astype(jnp.float32) / total
    keep = (waves[None, :] < limits[:, None]).astype(jnp.float32)
    values = decay * factor[None, :] * keep
    return jnp.concatenate([values, values], axis=1)


def reference(first_rhs, innovations, start_mult, trajectory, weight_in, weight_out, vertical_modes, length_scale, band_limit, obs_col, obs_count, obs_var):
    slopes = 1.0 - jnp.tanh(jnp.einsum("hd,sdc->shc", weight_in, trajectory.astype(jnp.float32), precision=HIGH)) ** 2

    def tangent(field):
        inner = jnp.einsum("hd,sdc->shc", weight_in, field, precision=HIGH)
        return field + jnp.einsum("dh,shc->sdc", weight_out, slopes * inner, precision=HIGH)

    def adjoint(field):
        inner = jnp.einsum("dh,sdc->shc", weight_out, field, precision=HIGH)
        return field + jnp.einsum("hd,shc->sdc", weight_in, slopes * inner, precision=HIGH)

    def apply_lower(field):
        moved = tangent(field)[:-1]
        return field - jnp.concatenate([jnp.zeros_like(field[:1]), moved], axis=0)

    def apply_upper(field):
        later = jnp.concatenate([field[1:], jnp.zeros_like(field[:1])], axis=0)
        return field - adjoint(later)

    table = spectral_table(jnp.arange(COLS, dtype=jnp.int32), KW, COLS)
    spec = spectrum(length_scale, band_limit, COLS, KW)

    def covariance(field):
        modes = jnp.einsum("md,sdc->smc", vertical_modes, field, precision=HIGH)
        coeffs = jnp.einsum("smc,ck->smk", modes, table, precision=HIGH) * spec[None]
        back = jnp.einsum("smk,ck->smc", coeffs, table, precision=HIGH)
        return jnp.einsum("md,smc->sdc", vertical_modes, back, precision=HIGH)

    slot_ids = jnp.arange(SLOTS, dtype=jnp.int32)
    live = ((slot_ids % OBS_DEV)[None, :] < obs_count[:, slot_ids // OBS_DEV]).astype(jnp.float32)

    def observe(field):
        picked = jnp.take_along_axis(field, obs_col[:, None, :], axis=2)
        return jnp.transpose(picked, (0, 2, 1)) * live[:, :, None]

    def spread(values):
        masked = values * live[:, :, None]
        blank = jnp.zeros((SUBS, D, COLS), jnp.float32)
        return jax.vmap(lambda target, where_at, items: target.at[:, where_at].add(items.T))(blank, obs_col, masked)

    def later_sums(field):
        return jnp.flip(jnp.cumsum(jnp.flip(field, 0), axis=0), 0)

    def earlier_sums(field):
        return jnp.cumsum(field, axis=0)

    multiplier = start_mult
    obs_multiplier = jnp.zeros_like(innovations)
    increment = jnp.zeros_like(start_mult)
    res_mult = first_rhs - covariance(start_mult)
    res_obs = innovations
    res_state = -apply_upper(start_mult)
    for sweep in range(ITERS):
        dir_mult = later_sums(res_state)
        cov_mult = covariance(dir_mult)
        dir_state = earlier_sums(res_mult - cov_mult)
        dir_obs = res_obs / obs_var[:, :, None]
        image_mult = cov_mult + apply_lower(dir_state)
        image_obs = obs_var[:, :, None] * dir_obs + observe(dir_state)
        image_state = apply_upper(dir_mult) + spread(dir_obs)
        upper = jnp.sum(image_mult * res_mult) + jnp.sum(image_obs * res_obs) + jnp.sum(image_state * res_state)
        lower = jnp.sum(image_mult * image_mult) + jnp.sum(image_obs * image_obs) + jnp.sum(image_state * image_state)
        alpha = upper / lower
        multiplier = multiplier + alpha * dir_mult
        obs_multiplier = obs_multiplier + alpha * dir_obs
        increment = increment + alpha * dir_state
        res_mult = res_mult - alpha * image_mult
        res_obs = res_obs - alpha * image_obs
        res_state = res_state - alpha * image_state
    return multiplier, obs_multiplier, increment
```

```python
import math

import jax
import jax.numpy as jnp
import numpy as np
from jax import lax
from jax.experimental import pallas as pl
from jax.experimental.pallas import tpu as pltpu
from jax.sharding import PartitionSpec as P

KW = 128
SUBS = 8
COLN = 16
GRPS = 2
RING = SUBS * GRPS
PAD = 24
MESH = pl.DeviceIdType.MESH
HIGH = lax.Precision.HIGH
F32 = jnp.float32
BF16 = jnp.bfloat16
WIDE = 128


def dot_dims(left, right, dims):
    return lax.dot_general(
        left, right, (dims, ((), ())), precision=HIGH, preferred_element_type=F32
    )


def product(left, right):
    return dot_dims(left, right, ((1,), (0,)))


def product_first(left, right):
    return dot_dims(left, right, ((0,), (0,)))


def dot3(x, high, low, dims):
    x_high = x.astype(BF16)
    x_low = (x - x_high.astype(F32)).astype(BF16)

    def one(a, b):
        return lax.dot_general(a, b, (dims, ((), ())), preferred_element_type=F32)

    return one(x_high, high) + (one(x_high, low) + one(x_low, high))


def spectral_tables(total):
    phase = np.arange(total)[:, None] * np.arange(KW)[None, :] % total
    angle = 2.0 * math.pi / total * phase
    table = np.concatenate([np.cos(angle), np.sin(angle)], axis=1).astype(np.float32)
    high = table.astype(jnp.bfloat16)
    low = (table - high.astype(np.float32)).astype(jnp.bfloat16)
    return high, low


def spectrum(scales, limits, total, count):
    waves = jnp.arange(count, dtype=jnp.int32)
    wavef = waves.astype(F32)
    decay = jnp.exp(-0.5 * (2.0 * math.pi * wavef[None, :] * scales[:, None] / total) ** 2)
    factor = jnp.where(waves == 0, 1.0, 2.0).astype(F32) / total
    keep = (waves[None, :] < limits[:, None]).astype(F32)
    values = decay * factor[None, :] * keep
    return jnp.concatenate([values, values], axis=1)


class Exchange:
    def __init__(self, group, sems, row, src_of, dst_of):
        self.group, self.sems, self.row = group, sems, row
        self.src_of, self.dst_of = src_of, dst_of

    def copy(self, peer, slot):
        return pltpu.make_async_remote_copy(
            src_ref=self.src_of(peer),
            dst_ref=self.dst_of(slot),
            send_sem=self.sems.at[2 * self.row, peer],
            recv_sem=self.sems.at[2 * self.row + 1, slot],
            device_id=self.group.device(peer),
            device_id_type=MESH,
        )

    def each(self, act):
        group = self.group

        def step(k, carry):
            act(lax.rem(group.me + k, group.count))
            return carry

        lax.fori_loop(1, group.count, step, 0)

    def start(self):
        self.each(lambda peer: self.copy(peer, self.group.me).start())

    def wait_recv(self):
        self.each(lambda peer: self.copy(peer, peer).wait_recv())

    def wait_send(self):
        self.each(lambda peer: self.copy(peer, peer).wait_send())


class RingGroup:
    count = RING

    def __init__(self):
        self.me = lax.axis_index("sub") * GRPS + lax.axis_index("grp")

    def device(self, peer):
        return {"sub": lax.div(peer, GRPS), "grp": lax.rem(peer, GRPS)}


class SubGroup:
    count = SUBS

    def __init__(self):
        self.me = lax.axis_index("sub")

    def device(self, peer):
        return {"sub": peer}


class ColGroup:
    count = COLN

    def __init__(self):
        self.me = lax.axis_index("col")

    def device(self, peer):
        return {"col": peer}


class PairGroup:
    count = GRPS

    def __init__(self):
        self.me = lax.axis_index("grp")

    def device(self, peer):
        return {"grp": peer}


def greet(*groups):
    barrier = pltpu.get_barrier_semaphore()
    total = 0
    for group in groups:

        def step(k, carry, group=group):
            peer = lax.rem(group.me + k, group.count)
            pl.semaphore_signal(
                barrier, inc=1, device_id=group.device(peer), device_id_type=MESH
            )
            return carry

        lax.fori_loop(1, group.count, step, 0)
        total += group.count - 1
    pl.semaphore_wait(barrier, total)


def lanes(index):
    return pl.ds(pl.multiple_of(index * WIDE, WIDE), WIDE)


def pair_sums(buffer, into):
    for t in range(SUBS):
        into[t] = buffer[2 * t] + buffer[2 * t + 1]


def suffix_sums(rows, into):
    total = rows[SUBS - 1]
    into[SUBS - 1] = total
    for t in range(SUBS - 2, -1, -1):
        total = total + rows[t]
        into[t] = total


def next_sub(peer):
    return lax.rem(lax.div(peer, GRPS) + 1, SUBS)


COEF = ((1,), (0,))
BACK = ((1,), (1,))


def first_kernel(np_ref, am, thi, tlo, spec, mup, mt, cl, buf, cbuf, nt, sems):
    ring, cols, pair = RingGroup(), ColGroup(), PairGroup()
    s, r, c, g = lax.axis_index("sub"), ring.me, cols.me, pair.me
    greet(ring, cols)
    fwd = Exchange(ring, sems, 0, lambda p: np_ref.at[p], lambda i: buf.at[i])
    amp = Exchange(cols, sems, 1, lambda p: am.at[p], lambda i: cbuf.at[:, lanes(i)])
    ret = Exchange(ring, sems, 2, lambda p: mt.at[next_sub(p)], lambda i: mup.at[i])
    coef = Exchange(pair, sems, 3, lambda p: cl.at[g], lambda i: cl.at[i])
    fwd.start()
    amp.start()
    buf[r] = np_ref[r]
    cbuf[:, lanes(c)] = am[c]
    fwd.wait_recv()
    pair_sums(buf, nt)
    suffix_sums(nt, mt)
    ret.start()
    mup[r] = mt[lax.rem(s + 1, SUBS)]
    amp.wait_recv()
    cl[g] = dot3(cbuf[...], thi[...], tlo[...], COEF) * spec[...]
    coef.start()
    coef.wait_recv()
    ret.wait_recv()
    for one in (fwd, amp, ret, coef):
        one.wait_send()


def middle_kernel(second, *refs):
    if second:
        (am, fp, h0, h1, rt, thi, tlo, spec,
         bk, up, full, ft, h0t, h1t,
         buf, cbuf, gbuf, wide, sct, sems) = refs
    else:
        (am, fp, h0, rt, cl, thi, tlo, spec,
         bk, up, full, ft, h0t, bl, sb, m2t,
         buf, cbuf, gbuf, wide, sct, lwide, sems) = refs
    ring, subs, cols = RingGroup(), SubGroup(), ColGroup()
    s, r, c = lax.axis_index("sub"), ring.me, cols.me
    g = lax.axis_index("grp")
    greet(ring, cols)
    amp = Exchange(cols, sems, 0, lambda p: am.at[p], lambda i: cbuf.at[:, lanes(i)])
    fwd = Exchange(ring, sems, 1, lambda p: fp.at[p], lambda i: buf.at[i])
    gat = Exchange(ring, sems, 2, lambda p: gbuf.at[r], lambda i: gbuf.at[i])
    bak = Exchange(cols, sems, 3, lambda p: wide.at[:, lanes(p)], lambda i: bk.at[i])
    hf0 = Exchange(subs, sems, 4, lambda p: h0.at[p * GRPS + g], lambda i: h0t.at[i])
    ful = Exchange(ring, sems, 5, lambda p: rt.at[lax.div(p, GRPS)], lambda i: full.at[i])
    if second:
        hf1 = Exchange(subs, sems, 6, lambda p: h1.at[p * GRPS + g], lambda i: h1t.at[i])
        ret = Exchange(ring, sems, 7, lambda p: sct.at[lax.div(p, GRPS)], lambda i: up.at[i])
        every = (amp, fwd, gat, bak, hf0, ful, hf1, ret)
    else:
        lba = Exchange(cols, sems, 6, lambda p: lwide.at[:, lanes(p)], lambda i: bl.at[i])
        ret = Exchange(ring, sems, 7, lambda p: m2t.at[next_sub(p)], lambda i: up.at[i])
        sbr = Exchange(ring, sems, 8, lambda p: sct.at[lax.div(p, GRPS)], lambda i: sb.at[i])
        every = (amp, fwd, gat, bak, hf0, ful, lba, ret, sbr)
    amp.start()
    fwd.start()
    cbuf[:, lanes(c)] = am[c]
    buf[r] = fp[r]
    h0t[s] = h0[r]
    full[r] = rt[s]
    if second:
        h1t[s] = h1[r]
    else:
        lwide[...] = dot3(cl[...].reshape(GRPS * PAD, 2 * KW), thi[...], tlo[...], BACK)
        lba.start()
        bl[c] = lwide[:, lanes(c)]
    amp.wait_recv()
    gbuf[r] = dot3(cbuf[...], thi[...], tlo[...], COEF) * spec[...]
    gat.start()
    fwd.wait_recv()
    pair_sums(buf, ft)
    if second:
        total = jnp.zeros_like(ft[0])
        for t in range(SUBS):
            sct[t] = total
            total = total + ft[t]
        ret.start()
        up[r] = sct[s]
    else:
        suffix_sums(ft, m2t)
        ret.start()
        up[r] = m2t[lax.rem(s + 1, SUBS)]
    hf0.start()
    if second:
        hf1.start()
    gat.wait_recv()
    parts = []
    for h in range(GRPS):
        total = gbuf[GRPS * (SUBS - 1) + h]
        for u in range(SUBS - 1):
            total = total + jnp.where(u + 1 <= s, 1.0, 0.0) * gbuf[GRPS * u + h]
        parts.append(total)
    wide[...] = dot3(jnp.concatenate(parts, axis=0), thi[...], tlo[...], BACK)
    bak.start()
    bk[c] = wide[:, lanes(c)]
    hf0.wait_recv()
    if second:
        ful.start()
        hf1.wait_recv()
    else:
        total = h0t[0]
        sct[0] = total
        for t in range(1, SUBS):
            total = total + h0t[t]
            sct[t] = total
        sbr.start()
        sb[r] = sct[s]
        ful.start()
        lba.wait_recv()
        sbr.wait_recv()
    ret.wait_recv()
    bak.wait_recv()
    ful.wait_recv()
    for one in every:
        one.wait_send()


def fold(x):
    return jnp.sum(x.reshape(x.shape[0] // 8, 8, x.shape[1]), axis=0)


def last_kernel(tp, ap, r1t, l0t, mt, et, t1t, og, out, tbuf, abuf, red1, red2, sems):
    ring, cols = RingGroup(), ColGroup()
    r, c = ring.me, cols.me
    greet(ring, cols)
    first = Exchange(ring, sems, 0, lambda p: tp.at[p], lambda i: tbuf.at[i])
    other = Exchange(ring, sems, 1, lambda p: ap.at[p], lambda i: abuf.at[i])
    one = Exchange(ring, sems, 2, lambda p: red1.at[r], lambda i: red1.at[i])
    two = Exchange(cols, sems, 3, lambda p: red2.at[c], lambda i: red2.at[i])
    first.start()
    other.start()
    tbuf[r] = tp[r]
    abuf[r] = ap[r]
    first.wait_recv()
    other.wait_recv()
    zero = jnp.zeros((8, WIDE), F32)
    sums = [zero] * 6

    def gather(x0, x1, x2):
        d0, d1 = x0 - x1, x1 - x2
        terms = (d0 * x0, d0 * d0, d0 * x1 + d1 * x0, d1 * x1, d0 * d1, d1 * d1)
        for i, term in enumerate(terms):
            sums[i] = sums[i] + fold(term)

    for t in range(SUBS):
        blank = jnp.zeros_like(mt[0])
        x1 = t1t[t - 1] if t else blank
        x2 = tbuf[2 * t - 2] + tbuf[2 * t - 1] if t else blank
        gather(r1t[t], x1, x2)
        here = mt[t] - l0t[t]
        later = mt[t + 1] - l0t[t + 1] if t < SUBS - 1 else blank
        gather(here - later, et[t], abuf[2 * t] + abuf[2 * t + 1])
    rows = [jnp.sum(x, axis=0, keepdims=True) for x in sums]
    rows = rows + [jnp.zeros((1, WIDE), F32)] * 2
    red1[r] = jnp.concatenate(rows, axis=0) + og[...]
    one.start()
    one.wait_recv()
    total = red1[0]
    for i in range(1, RING):
        total = total + red1[i]
    red2[c] = total
    two.start()
    two.wait_recv()
    total = red2[0]
    for i in range(1, COLN):
        total = total + red2[i]
    out[...] = total
    for x in (first, other, one, two):
        x.wait_send()


def call(kernel, name, ident, outs, scratch, sems, args):
    vmem = pl.BlockSpec(memory_space=pltpu.VMEM)
    return pl.pallas_call(
        kernel,
        name=name,
        out_shape=[jax.ShapeDtypeStruct(shape, F32) for shape in outs],
        in_specs=[vmem] * len(args),
        out_specs=[vmem] * len(outs),
        scratch_shapes=[pltpu.VMEM(shape, F32) for shape in scratch]
        + [pltpu.SemaphoreType.DMA((2 * sems, 16))],
        compiler_params=pltpu.CompilerParams(collective_id=ident, has_side_effects=True),
    )(*args)


def on_device(
    first_rhs,
    innovations,
    start_mult,
    trajectory,
    weight_in,
    weight_out,
    vertical_modes,
    length_scale,
    band_limit,
    obs_col,
    obs_count,
    obs_var,
):
    first_rhs, innovations, start_mult = first_rhs[0], innovations[0], start_mult[0]
    var = obs_var[0][:, None]
    deep, width = first_rhs.shape
    s, c, g = lax.axis_index("sub"), lax.axis_index("col"), lax.axis_index("grp")
    total_cols = width * COLN
    half = vertical_modes.shape[0]
    owned = half // COLN
    piece = deep // RING
    field = (RING, piece, width)
    every = (SUBS, piece, width)
    amps = (COLN, PAD, width)
    both = (COLN, GRPS * PAD, width)
    thi, tlo = (jnp.asarray(x) for x in spectral_tables(total_cols))

    later_mult = lax.ppermute(start_mult, "sub", [((i + 1) % SUBS, i) for i in range(SUBS)])
    modes = jnp.pad(vertical_modes.reshape(COLN, owned, deep), ((0, 0), (0, PAD - owned), (0, 0)))
    other_modes = lax.ppermute(modes, "grp", [(0, 1), (1, 0)])
    modes_low = jnp.where(g == 0, modes, other_modes)
    modes_high = jnp.where(g == 0, other_modes, modes)
    all_modes = jnp.stack([modes_low, modes_high], axis=1).reshape(COLN * GRPS * PAD, deep)
    modes = modes.reshape(COLN * PAD, deep)

    first_mode = g * half + c * owned
    scales = lax.dynamic_slice_in_dim(length_scale, first_mode, owned, 0)
    limits = lax.dynamic_slice_in_dim(band_limit, first_mode, owned, 0)
    spec = jnp.pad(spectrum(scales, limits, total_cols, KW), ((0, PAD - owned), (0, 0)))

    slopes = 1.0 - jnp.tanh(product(weight_in, trajectory[0].astype(F32))) ** 2
    has_later = (s < SUBS - 1).astype(F32)
    leads = (g == 0).astype(F32)

    def tangent(z):
        return product(weight_out, slopes * product(weight_in, z))

    def adjoint(z):
        return product_first(weight_in, slopes * product_first(weight_out, z)) * has_later

    def amplitudes(z):
        return product(modes, z).reshape(amps)

    def restored(back):
        return product_first(all_modes, back.reshape(COLN * GRPS * PAD, width))

    local_cols = obs_col[0] - c * width
    slot_ids = jnp.arange(local_cols.shape[0], dtype=jnp.int32)
    live = (slot_ids < obs_count[0, 0]).astype(F32)
    pick = (jnp.arange(width, dtype=jnp.int32)[:, None] == local_cols[None, :]).astype(F32)
    pick = pick * live[None, :]

    def observe(z):
        return dot_dims(pick, z, ((0,), (1,)))

    def spread(values):
        return dot_dims(values, pick, ((0,), (1,)))

    n0 = adjoint(later_mult).reshape(field)
    m_up, m_all, start_coef = call(
        first_kernel, "first_exchange", 0,
        [field, every, (GRPS, PAD, 2 * KW)],
        [field, (PAD, total_cols), every], 4,
        [n0, amplitudes(start_mult), thi, tlo, spec],
    )
    m_up = m_up.reshape(deep, width)
    dir_obs = innovations / var
    e = adjoint(m_up - later_mult * has_later) - leads * spread(dir_obs)
    back, m2_up, m_full, e_all, rhs_all, start_back, rhs_sum, m2_all = call(
        lambda *refs: middle_kernel(False, *refs), "middle_exchange", 1,
        [both, field, field, every, every, both, field, every],
        [field, (PAD, total_cols), (RING, PAD, 2 * KW), (GRPS * PAD, total_cols), every,
         (GRPS * PAD, total_cols)], 9,
        [amplitudes(m_up), e.reshape(field), first_rhs.reshape(field), m_all, start_coef,
         thi, tlo, spec],
    )
    m2_up = m2_up.reshape(deep, width)
    dir_state = rhs_sum.reshape(deep, width) - restored(back)
    res_mult = first_rhs - restored(start_back)
    seen = observe(dir_state)
    moved = tangent(dir_state)
    back2, moved_sum, m2_full, moved_all, res_all, start_all = call(
        lambda *refs: middle_kernel(True, *refs), "second_exchange", 2,
        [both, field, field, every, every, every],
        [field, (PAD, total_cols), (RING, PAD, 2 * KW), (GRPS * PAD, total_cols), every], 8,
        [amplitudes(m2_up), moved.reshape(field), res_mult.reshape(field),
         start_mult.reshape(field), m2_all, thi, tlo, spec],
    )
    q = moved_sum.reshape(deep, width) - restored(back2)
    a2 = adjoint(m2_up) + leads * spread(seen / var)
    t2 = tangent(q)
    seen2 = observe(q)
    x0, x1, x2 = innovations, -seen, -seen2
    d0, d1 = x0 - x1, x1 - x2
    terms = (d0 * x0, d0 * d0, d0 * x1 + d1 * x0, d1 * x1, d0 * d1, d1 * d1)
    obs_sums = [jnp.sum(x.reshape(-1, WIDE), axis=0) for x in terms]
    obs_sums = jnp.stack(obs_sums + [jnp.zeros((WIDE,), F32)] * 2) * leads
    (sums,) = call(
        last_kernel, "last_exchange", 3,
        [(8, WIDE)],
        [field, field, (RING, 8, WIDE), (COLN, 8, WIDE)], 4,
        [t2.reshape(field), a2.reshape(field), res_all, start_all, m_all, e_all, moved_all,
         obs_sums],
    )
    gram = jnp.sum(sums, axis=1)
    a = gram[0] / gram[1]
    b = 1.0 - a
    upper = b * b * gram[0] + a * b * gram[2] + a * a * gram[3]
    lower = b * b * gram[1] + 2.0 * a * b * gram[4] + a * a * gram[5]
    a_next = upper / lower
    dir_mult = m_full.reshape(deep, width) - start_mult
    next_mult = b * dir_mult + a * m2_full.reshape(deep, width)
    next_state = b * dir_state + a * q
    next_obs = (b * innovations - a * seen) / var
    multiplier = start_mult + a * dir_mult + a_next * next_mult
    obs_multiplier = a * dir_obs + a_next * next_obs
    increment = a * dir_state + a_next * next_state
    return multiplier[None], obs_multiplier[None], increment[None]


def solution(mesh):
    in_specs = (
        P("sub", None, "col"),
        P("sub", "col", None),
        P("sub", None, "col"),
        P("sub", None, "col"),
        P("grp", None),
        P(None, "grp"),
        P("grp", None),
        P(),
        P(),
        P("sub", "col"),
        P("sub", "col"),
        P("sub", "col"),
    )
    out_specs = (P("sub", None, "col"), P("sub", "col", None), P("sub", None, "col"))
    return jax.shard_map(
        on_device, mesh=mesh, in_specs=in_specs, out_specs=out_specs, check_vma=False
    )
```

```python
import math
import types

import jax
import jax.numpy as jnp
import numpy as np
from jax import lax
from jax.experimental import pallas as pl
from jax.experimental.pallas import tpu as pltpu
from jax.sharding import PartitionSpec as P

KW = 128
SUBS = 8
COLN = 16
GRPS = 2
CORES = 2
RING = SUBS * GRPS
PAD = 24
WIDE = 128
CHUNK = 256
MESH = pl.DeviceIdType.MESH
F32 = jnp.float32
BF16 = jnp.bfloat16
ROWS = ((1,), (0,))
BACK = ((1,), (1,))


def spectral_tables(total):
    phase = np.arange(total)[:, None] * np.arange(KW)[None, :] % total
    angle = 2.0 * math.pi / total * phase
    table = np.concatenate([np.cos(angle), np.sin(angle)], axis=1).astype(np.float32)
    high = table.astype(jnp.bfloat16)
    low = (table - high.astype(np.float32)).astype(jnp.bfloat16)
    return high, low


def spectrum(scales, limits, total, count):
    waves = jnp.arange(count, dtype=jnp.int32)
    wavef = waves.astype(F32)
    decay = jnp.exp(-0.5 * (2.0 * math.pi * wavef[None, :] * scales[:, None] / total) ** 2)
    factor = jnp.where(waves == 0, 1.0, 2.0).astype(F32) / total
    keep = (waves[None, :] < limits[:, None]).astype(F32)
    values = decay * factor[None, :] * keep
    return jnp.concatenate([values, values], axis=1)


class Group:
    def __init__(self, me, count, device):
        self.me, self.count, self.device = me, count, device


class Exchange:
    def __init__(self, group, sems, row, src_of, dst_of):
        self.group, self.sems, self.row = group, sems, row
        self.src_of, self.dst_of = src_of, dst_of

    def copy(self, peer, slot):
        return pltpu.make_async_remote_copy(
            src_ref=self.src_of(peer),
            dst_ref=self.dst_of(slot),
            send_sem=self.sems.at[2 * self.row, peer],
            recv_sem=self.sems.at[2 * self.row + 1, slot],
            device_id=self.group.device(peer),
            device_id_type=MESH,
        )

    def each(self, act):
        group = self.group

        def step(k, carry):
            act(lax.rem(group.me + k, group.count))
            return carry

        lax.fori_loop(1, group.count, step, 0)

    def start(self):
        self.each(lambda peer: self.copy(peer, self.group.me).start())

    def wait_recv(self):
        self.each(lambda peer: self.copy(peer, peer).wait_recv())

    def wait_send(self):
        self.each(lambda peer: self.copy(peer, peer).wait_send())


def greet(*groups):
    barrier = pltpu.get_barrier_semaphore()
    total = 0
    for group in groups:

        def step(k, carry, group=group):
            peer = lax.rem(group.me + k, group.count)
            pl.semaphore_signal(
                barrier, inc=1, device_id=group.device(peer), device_id_type=MESH
            )
            return carry

        lax.fori_loop(1, group.count, step, 0)
        total += group.count - 1
    pl.semaphore_wait(barrier, total)


def lanes(index):
    return pl.ds(pl.multiple_of(index * WIDE, WIDE), WIDE)


def chunk(index, size=CHUNK):
    return pl.ds(pl.multiple_of(index * size, size), size)


def split(x):
    high = x.astype(BF16)
    return high, (x - high.astype(F32)).astype(BF16)


def mm(a, b, dims):
    return lax.dot_general(a, b, (dims, ((), ())), preferred_element_type=F32)


def mm3(a, b, dims):
    return mm(a[0], b[0], dims) + (mm(a[0], b[1], dims) + mm(a[1], b[0], dims))


def pair_sums(buffer, into):
    for t in range(SUBS):
        into[t] = buffer[2 * t] + buffer[2 * t + 1]


def suffix_sums(rows, into):
    total = rows[SUBS - 1]
    into[SUBS - 1] = total
    for t in range(SUBS - 2, -1, -1):
        total = total + rows[t]
        into[t] = total


def prefix_sums(rows, into):
    total = rows[0]
    into[0] = total
    for t in range(1, SUBS):
        total = total + rows[t]
        into[t] = total


def lagged_sums(rows, into):
    total = jnp.zeros_like(rows[0])
    for t in range(SUBS):
        into[t] = total
        total = total + rows[t]


def fold(x):
    return jnp.sum(x.reshape(x.shape[0] // 8, 8, x.shape[1]), axis=0)


class Sums:
    def __init__(self):
        self.held = None

    def add(self, x0, x1, x2, scale=None):
        d0, d1 = x0 - x1, x1 - x2
        terms = (d0 * x0, d0 * d0, d0 * x1 + d1 * x0, d1 * x1, d0 * d1, d1 * d1)
        terms = [fold(x) for x in terms]
        if scale is not None:
            terms = [x * scale for x in terms]
        self.held = terms if self.held is None else [a + b for a, b in zip(self.held, terms)]

    def tile(self):
        rows = [jnp.sum(x, axis=0, keepdims=True) for x in self.held]
        return jnp.concatenate(rows + [jnp.zeros((1, WIDE), F32)] * 2, axis=0)


INPUTS = (
    "b", "obs", "l0", "traj", "w_in", "w_out", "modes", "thi", "tlo", "spec", "pick", "pick_t",
    "var",
)
OUTPUTS = ("mult", "obs_mult", "incr")
NAMES = (
    "shift", "vpair", "vz", "vcore", "hl", "hb", "hr", "nfw", "mret", "sret", "mful", "efw",
    "m2ret", "tfw", "qret", "m2ful", "afw", "ufw", "gat1", "gat2", "red1", "amp0", "lba", "amp1",
    "bak1", "amp2", "bak2", "red2", "clx",
)


def scratch_list(deep, width, hidden, total_cols):
    piece = deep // RING
    field, every = (RING, piece, width), (SUBS, piece, width)
    amps, flat = (COLN, PAD, width), (PAD, total_cols)
    coef, wide = (RING, PAD, 2 * KW), (GRPS, PAD, total_cols)
    back = (COLN, GRPS, PAD, width)
    out = {
        "fin": ((hidden, deep), F32), "fout": ((deep, hidden), F32),
        "wih": ((hidden, deep), BF16), "wil": ((hidden, deep), BF16),
        "woh": ((deep, hidden), BF16), "wol": ((deep, hidden), BF16),
        "slp": ((width, hidden), F32), "hh": ((width, hidden), BF16), "hl_": ((width, hidden), BF16),
        "zh": ((width, deep), BF16), "zl": ((width, deep), BF16), "ot": ((width, deep), F32),
        "vpad": ((COLN, PAD, deep), F32), "voth": ((COLN // CORES, CORES, PAD, deep), F32),
        "vah": ((GRPS, COLN * PAD, deep), BF16), "val": ((GRPS, COLN * PAD, deep), BF16),
        "seen": ((64, deep), F32), "seen2": ((64, deep), F32), "p3t": ((width, deep), F32),
        "ht": ((width, deep), F32), "qt": ((width, deep), F32),
        "cl": ((GRPS, PAD, 2 * KW), F32),
        "r1": (field, F32), "p3": (field, F32), "q": (field, F32),
        "rb1": ((RING, 8, WIDE), F32), "rb2": ((COLN, 8, WIDE), F32),
    }
    for name in ("lup", "np_", "nbuf", "mup", "sb", "mfull", "ep", "ebuf", "m2up", "tp", "tbuf",
                 "qs", "m2full", "ap", "abuf", "up", "ubuf"):
        out[name] = (field, F32)
    for name in ("nt", "mt", "bt", "sbt", "l0t", "r1t", "et", "m2t", "t1t", "qst"):
        out[name] = (every, F32)
    for i in range(3):
        out[f"am{i}"] = (amps, F32)
        out[f"cb{i}"] = (flat, F32)
        out[f"wd{i}"] = (wide, F32)
        out[f"bk{i}"] = (back, F32)
    for i in (1, 2):
        out[f"gb{i}"] = (coef, F32)
    return out


def kernel(names, *refs):
    x = types.SimpleNamespace(**dict(zip(names, refs)))
    s, c, g = lax.axis_index("sub"), lax.axis_index("col"), lax.axis_index("grp")
    core, z = lax.rem(c, CORES), lax.div(c, CORES)
    r = s * GRPS + g
    deep, hidden, width = x.woh.shape[0], x.woh.shape[1], x.slp.shape[0]
    ring = Group(r, RING, lambda p: {"sub": lax.div(p, GRPS), "grp": lax.rem(p, GRPS)})
    subs = Group(s, SUBS, lambda p: {"sub": p})
    cols = Group(c, COLN, lambda p: {"col": p})
    pair = Group(g, GRPS, lambda p: {"grp": p})
    same = Group(z, COLN // CORES, lambda p: {"col": p * CORES + core})
    chip = Group(core, CORES, lambda p: {"col": z * CORES + p})

    def over(name, group, src, dst):
        return Exchange(group, x.sems, NAMES.index(name), src, dst)

    def next_sub(p):
        return lax.rem(lax.div(p, GRPS) + 1, SUBS)

    def forward(name, src, dst):
        return over(name, ring, lambda p: src.at[p], lambda i: dst.at[i])

    def giving(name, src, dst):
        return over(name, ring, lambda p: src.at[lax.div(p, GRPS)], lambda i: dst.at[i])

    def giving_next(name, src, dst):
        return over(name, ring, lambda p: src.at[next_sub(p)], lambda i: dst.at[i])

    def halves(name, src, dst):
        return over(name, subs, lambda p: src.at[p * GRPS + g], lambda i: dst.at[i])

    def amps(name, src, dst):
        return over(name, cols, lambda p: src.at[p], lambda i: dst.at[:, lanes(i)])

    def backs(name, src, dst):
        return over(name, cols, lambda p: src.at[:, :, lanes(p)], lambda i: dst.at[i])

    def gathers(name, buf):
        return over(name, ring, lambda p: buf.at[r], lambda i: buf.at[i])

    row = NAMES.index("shift")
    shift = pltpu.make_async_remote_copy(
        src_ref=x.l0, dst_ref=x.lup, send_sem=x.sems.at[2 * row, 0],
        recv_sem=x.sems.at[2 * row + 1, 0],
        device_id={"sub": lax.rem(s + SUBS - 1, SUBS)}, device_id_type=MESH,
    )
    vpair = over("vpair", pair, lambda p: x.vpad.at[c], lambda i: x.voth.at[z, core])
    vz = over("vz", same, lambda p: x.voth.at[z, core], lambda i: x.voth.at[i, core])
    vcore = over("vcore", chip, lambda p: x.voth.at[:, core], lambda i: x.voth.at[:, i])
    hl = halves("hl", x.l0, x.l0t)
    hb = halves("hb", x.b, x.bt)
    hr = halves("hr", x.r1, x.r1t)
    nfw = forward("nfw", x.np_, x.nbuf)
    mret = giving_next("mret", x.mt, x.mup)
    sret = giving("sret", x.sbt, x.sb)
    mful = giving("mful", x.mt, x.mfull)
    efw = forward("efw", x.ep, x.ebuf)
    m2ret = giving_next("m2ret", x.m2t, x.m2up)
    tfw = forward("tfw", x.tp, x.tbuf)
    qret = giving("qret", x.qst, x.qs)
    m2ful = giving("m2ful", x.m2t, x.m2full)
    afw = forward("afw", x.ap, x.abuf)
    ufw = forward("ufw", x.up, x.ubuf)
    gat1, gat2 = gathers("gat1", x.gb1), gathers("gat2", x.gb2)
    red1 = gathers("red1", x.rb1)
    red2 = over("red2", cols, lambda p: x.rb2.at[c], lambda i: x.rb2.at[i])
    amp0, amp1, amp2 = (amps(f"amp{i}", getattr(x, f"am{i}"), getattr(x, f"cb{i}")) for i in range(3))
    lba, bak1, bak2 = (
        backs(n, getattr(x, f"wd{i}"), getattr(x, f"bk{i}"))
        for i, n in enumerate(("lba", "bak1", "bak2"))
    )
    clx = over("clx", pair, lambda p: x.cl.at[g], lambda i: x.cl.at[i])
    sent = [vpair, vz, vcore, hl, hb, hr, nfw, mret, sret, mful, efw, m2ret, tfw, qret, m2ful,
            afw, ufw, gat1, gat2, red1, red2, amp0, amp1, amp2, lba, bak1, bak2, clx]

    get_in = pltpu.make_async_copy(x.w_in, x.fin, x.local.at[0])
    get_out = pltpu.make_async_copy(x.w_out, x.fout, x.local.at[1])
    get_in.start()
    get_out.start()

    def first_half(columns):
        weights = (x.woh, x.wol) if columns else (x.wih, x.wil)

        def step(j, carry):
            at = (slice(None), chunk(j)) if columns else (chunk(j), slice(None))
            pair_ = (weights[0][at], weights[1][at])
            value = mm3((x.zh[...], x.zl[...]), pair_, ROWS if columns else BACK)
            high, low = split(value * x.slp[:, chunk(j)])
            x.hh[:, chunk(j)] = high
            x.hl_[:, chunk(j)] = low
            return carry

        lax.fori_loop(0, hidden // CHUNK, step, 0)

    def second_half(columns):
        weights = (x.wih, x.wil) if columns else (x.woh, x.wol)

        def part(at):
            where = (slice(None), at) if columns else (at, slice(None))
            pair_ = (weights[0][where], weights[1][where])
            x.ot[:, at] = mm3((x.hh[...], x.hl_[...]), pair_, ROWS if columns else BACK)

        def step(j, carry):
            part(chunk(j))
            return carry

        lax.fori_loop(0, deep // CHUNK, step, 0)
        left = deep % CHUNK
        if left:
            part(pl.ds(deep - left, left))

    def adjoint(zt):
        x.zh[...], x.zl[...] = split(zt)
        first_half(True)
        second_half(True)
        return x.ot[...]

    def tangent(zt):
        x.zh[...], x.zl[...] = split(zt)
        first_half(False)
        second_half(False)
        return x.ot[...]

    def whole(ref):
        return ref[...].reshape(deep, width)

    def put(ref, value_t):
        ref[...] = value_t.T.reshape(ref.shape)

    def amplitudes(ref, into):
        value = mm3((x.vah[g], x.val[g]), split(whole(ref)), ROWS)
        into[...] = value.reshape(into.shape)

    def restored_t(bk):
        total = None
        for h in range(GRPS):
            turned = split(bk[:, h].reshape(COLN * PAD, width).T)
            term = mm3(turned, (x.vah[h], x.val[h]), ROWS)
            total = term if total is None else total + term
        return total

    tables = (x.thi, x.tlo)

    def coefficients(cb):
        return mm3(split(cb[...]), (x.thi[...], x.tlo[...]), ROWS) * x.spec[...]

    def spread_back(values, into):
        value = mm3(split(values), (x.thi[...], x.tlo[...]), BACK)
        into[...] = value.reshape(into.shape)

    def summed(gb):
        parts = []
        for h in range(GRPS):
            total = gb[GRPS * (SUBS - 1) + h]
            for u in range(SUBS - 1):
                total = total + jnp.where(u + 1 <= s, 1.0, 0.0) * gb[GRPS * u + h]
            parts.append(total)
        return jnp.concatenate(parts, axis=0)

    def pick_rows(vt):
        high, low = split(vt)
        return mm(x.pick_t[...], high, ROWS) + mm(x.pick_t[...], low, ROWS)

    def spread_rows(values):
        high, low = split(values)
        return mm(x.pick[...], high, ROWS) + mm(x.pick[...], low, ROWS)

    has_later = jnp.where(s < SUBS - 1, 1.0, 0.0)
    leads = jnp.where(g == 0, 1.0, 0.0)

    owned = x.modes.shape[0] // COLN
    for i in range(COLN):
        x.vpad[i, :owned] = x.modes[i * owned:(i + 1) * owned]
        x.vpad[i, owned:] = jnp.zeros((PAD - owned, deep), F32)
    greet(ring, cols)
    shift.start()
    vpair.start()
    hb.start()
    hl.start()
    x.bt[s] = x.b[r]
    x.l0t[s] = x.l0[r]
    traj_t = x.traj[...].astype(F32).T
    x.zh[...] = traj_t.astype(BF16)
    get_in.wait()

    def open_in(j, carry):
        high, low = split(x.fin[chunk(j), :])
        x.wih[chunk(j), :] = high
        x.wil[chunk(j), :] = low
        inner = mm(x.zh[...], high, BACK) + mm(x.zh[...], low, BACK)
        x.slp[:, chunk(j)] = 1.0 - jnp.tanh(inner) ** 2
        return carry

    lax.fori_loop(0, hidden // CHUNK, open_in, 0)
    get_out.wait()

    def open_out(j, carry):
        high, low = split(x.fout[chunk(j, 64), :])
        x.woh[chunk(j, 64), :] = high
        x.wol[chunk(j, 64), :] = low
        return carry

    lax.fori_loop(0, deep // 64, open_out, 0)
    high, low = split(x.vpad[...].reshape(COLN * PAD, deep))
    x.vah[g] = high
    x.val[g] = low
    shift.wait_recv()
    put(x.np_, adjoint(whole(x.lup).T) * has_later)
    nfw.start()
    x.nbuf[r] = x.np_[r]
    amplitudes(x.l0, x.am0)
    vpair.wait_recv()
    amp0.start()
    vz.start()
    x.cb0[:, lanes(c)] = x.am0[c]
    x.ht[...] = spread_rows(x.obs[...] / x.var[...])
    nfw.wait_recv()
    pair_sums(x.nbuf, x.nt)
    suffix_sums(x.nt, x.mt)
    mret.start()
    x.mup[r] = x.mt[lax.rem(s + 1, SUBS)]
    hb.wait_recv()
    prefix_sums(x.bt, x.sbt)
    sret.start()
    x.sb[r] = x.sbt[s]
    amp0.wait_recv()
    x.cl[g] = coefficients(x.cb0)
    mret.wait_recv()
    amplitudes(x.mup, x.am1)
    amp1.start()
    clx.start()
    x.cb1[:, lanes(c)] = x.am1[c]
    vz.wait_recv()
    vcore.start()
    put(x.ep, adjoint((whole(x.mup) - whole(x.lup)).T) * has_later - leads * x.ht[...])
    amp1.wait_recv()
    x.gb1[r] = coefficients(x.cb1)
    gat1.start()
    efw.start()
    x.ebuf[r] = x.ep[r]
    clx.wait_recv()
    spread_back(x.cl[...].reshape(GRPS * PAD, 2 * KW), x.wd0)
    vcore.wait_recv()
    high, low = split(x.voth[...].reshape(COLN * PAD, deep))
    x.vah[1 - g] = high
    x.val[1 - g] = low
    gat1.wait_recv()
    spread_back(summed(x.gb1), x.wd1)
    bak1.start()
    x.bk1[c] = x.wd1[:, :, lanes(c)]
    efw.wait_recv()
    pair_sums(x.ebuf, x.et)
    suffix_sums(x.et, x.m2t)
    m2ret.start()
    x.m2up[r] = x.m2t[lax.rem(s + 1, SUBS)]
    m2ret.wait_recv()
    amplitudes(x.m2up, x.am2)
    amp2.start()
    lba.start()
    x.cb2[:, lanes(c)] = x.am2[c]
    x.bk0[c] = x.wd0[:, :, lanes(c)]
    sret.wait_recv()
    bak1.wait_recv()
    p3t = whole(x.sb).T - restored_t(x.bk1)
    x.p3t[...] = p3t
    put(x.tp, tangent(p3t))
    tfw.start()
    x.tbuf[r] = x.tp[r]
    amp2.wait_recv()
    x.gb2[r] = coefficients(x.cb2)
    gat2.start()
    put(x.p3, x.p3t[...])
    x.seen[...] = pick_rows(x.p3t[...])
    tfw.wait_recv()
    pair_sums(x.tbuf, x.t1t)
    lagged_sums(x.t1t, x.qst)
    qret.start()
    x.qs[r] = x.qst[s]
    gat2.wait_recv()
    spread_back(summed(x.gb2), x.wd2)
    bak2.start()
    x.bk2[c] = x.wd2[:, :, lanes(c)]
    a2 = adjoint(whole(x.m2up).T) * has_later
    put(x.ap, a2 + leads * spread_rows(x.seen[...] / x.var[...]))
    afw.start()
    x.abuf[r] = x.ap[r]
    lba.wait_recv()
    x.r1[...] = x.b[...] - restored_t(x.bk0).T.reshape(x.r1.shape)
    hr.start()
    x.r1t[s] = x.r1[r]
    qret.wait_recv()
    bak2.wait_recv()
    qt = whole(x.qs).T - restored_t(x.bk2)
    x.qt[...] = qt
    put(x.up, tangent(qt))
    ufw.start()
    mful.start()
    m2ful.start()
    x.ubuf[r] = x.up[r]
    x.mfull[r] = x.mt[s]
    x.m2full[r] = x.m2t[s]
    put(x.q, x.qt[...])
    x.seen2[...] = pick_rows(x.qt[...])
    sums = Sums()
    for i in range(deep // WIDE):
        at = slice(i * WIDE, (i + 1) * WIDE)
        sums.add(x.obs[:, at], -x.seen[:, at], -x.seen2[:, at], leads)
    hl.wait_recv()
    afw.wait_recv()
    blank = jnp.zeros_like(x.mt[0])
    for t in range(SUBS):
        here = x.mt[t] - x.l0t[t]
        later = x.mt[t + 1] - x.l0t[t + 1] if t < SUBS - 1 else blank
        sums.add(here - later, x.et[t], x.abuf[2 * t] + x.abuf[2 * t + 1])
    hr.wait_recv()
    ufw.wait_recv()
    for t in range(SUBS):
        x1 = x.t1t[t - 1] if t else blank
        x2 = x.ubuf[2 * t - 2] + x.ubuf[2 * t - 1] if t else blank
        sums.add(x.r1t[t], x1, x2)
    x.rb1[r] = sums.tile()
    red1.start()
    red1.wait_recv()
    total = x.rb1[0]
    for i in range(1, RING):
        total = total + x.rb1[i]
    x.rb2[c] = total
    red2.start()
    mful.wait_recv()
    m2ful.wait_recv()
    red2.wait_recv()
    total = x.rb2[0]
    for i in range(1, COLN):
        total = total + x.rb2[i]
    gram = jnp.sum(total, axis=1, keepdims=True)
    gram = [gram[i:i + 1] for i in range(6)]
    a = gram[0] / gram[1]
    b = 1.0 - a
    upper = b * b * gram[0] + a * b * gram[2] + a * a * gram[3]
    lower = b * b * gram[1] + 2.0 * a * b * gram[4] + a * a * gram[5]
    a_next = upper / lower
    start = whole(x.l0)
    move = whole(x.mfull) - start
    mult = start + a * move + a_next * (b * move + a * whole(x.m2full))
    x.mult[...] = mult.reshape(x.mult.shape)
    p3 = whole(x.p3)
    x.incr[...] = (a * p3 + a_next * (b * p3 + a * whole(x.q))).reshape(x.incr.shape)
    obs = x.obs[...]
    x.obs_mult[...] = (a * obs + a_next * (b * obs - a * x.seen[...])) / x.var[...]
    for one in sent:
        one.wait_send()
    shift.wait_send()


def on_device(
    first_rhs,
    innovations,
    start_mult,
    trajectory,
    weight_in,
    weight_out,
    vertical_modes,
    length_scale,
    band_limit,
    obs_col,
    obs_count,
    obs_var,
):
    deep, width = first_rhs.shape[1:]
    slots = innovations.shape[1]
    hidden = weight_in.shape[0]
    c, g = lax.axis_index("col"), lax.axis_index("grp")
    total_cols = width * COLN
    half = vertical_modes.shape[0]
    owned = half // COLN
    field = (RING, deep // RING, width)
    thi, tlo = (jnp.asarray(x) for x in spectral_tables(total_cols))

    first_mode = g * half + c * owned
    scales = lax.dynamic_slice_in_dim(length_scale, first_mode, owned, 0)
    limits = lax.dynamic_slice_in_dim(band_limit, first_mode, owned, 0)
    spec = jnp.pad(spectrum(scales, limits, total_cols, KW), ((0, PAD - owned), (0, 0)))
    local_cols = obs_col[0] - c * width
    live = jnp.arange(slots, dtype=jnp.int32) < obs_count[0, 0]
    chosen = jnp.where(live, local_cols, -1)
    columns = jnp.arange(width, dtype=jnp.int32)
    pick = (columns[:, None] == chosen[None, :]).astype(BF16)
    pick_t = (chosen[:, None] == columns[None, :]).astype(BF16)

    vmem = pl.BlockSpec(memory_space=pltpu.VMEM)
    away = pl.BlockSpec(memory_space=pl.ANY)
    args = dict(
        b=first_rhs.reshape(field), obs=innovations[0], l0=start_mult.reshape(field),
        traj=trajectory[0], w_in=weight_in, w_out=weight_out, modes=vertical_modes,
        thi=thi, tlo=tlo, spec=spec, pick=pick, pick_t=pick_t, var=obs_var[0][:, None],
    )
    scratch = scratch_list(deep, width, hidden, total_cols)
    names = INPUTS + OUTPUTS + tuple(scratch) + ("local", "sems")
    shapes = (field, (slots, deep), field)
    mult, obs_mult, incr = pl.pallas_call(
        lambda *refs: kernel(names, *refs),
        name="saddle",
        out_shape=[jax.ShapeDtypeStruct(shape, F32) for shape in shapes],
        in_specs=[away if n in ("w_in", "w_out") else vmem for n in INPUTS],
        out_specs=[vmem] * len(shapes),
        scratch_shapes=[pltpu.VMEM(*scratch[n]) for n in scratch]
        + [pltpu.SemaphoreType.DMA((2,)), pltpu.SemaphoreType.DMA((2 * len(NAMES), 16))],
        compiler_params=pltpu.CompilerParams(collective_id=0, has_side_effects=True),
    )(*(args[n] for n in INPUTS))
    return (
        mult.reshape(1, deep, width), obs_mult[None], incr.reshape(1, deep, width)
    )


def solution(mesh):
    in_specs = (
        P("sub", None, "col"),
        P("sub", "col", None),
        P("sub", None, "col"),
        P("sub", None, "col"),
        P("grp", None),
        P(None, "grp"),
        P("grp", None),
        P(),
        P(),
        P("sub", "col"),
        P("sub", "col"),
        P("sub", "col"),
    )
    out_specs = (P("sub", None, "col"), P("sub", "col", None), P("sub", None, "col"))
    return jax.shard_map(
        on_device, mesh=mesh, in_specs=in_specs, out_specs=out_specs, check_vma=False
    )
```

```python
import math
import types

import jax
import jax.numpy as jnp
import numpy as np
from jax import lax
from jax.experimental import pallas as pl
from jax.experimental.pallas import tpu as pltpu
from jax.sharding import PartitionSpec as P

KW = 128
SUBS = 8
COLN = 16
GRPS = 2
CORES = 2
RING = SUBS * GRPS
PAD = 24
WIDE = 128
CHUNK = 256
MESH = pl.DeviceIdType.MESH
F32 = jnp.float32
BF16 = jnp.bfloat16
ROWS = ((1,), (0,))
BACK = ((1,), (1,))


def base_tables(total):
    waves = np.arange(KW)[None, :]
    inner, outer = np.arange(WIDE)[:, None], np.arange(0, total, WIDE)[:, None]
    parts = []
    for columns in (inner, outer):
        angle = 2.0 * math.pi / total * (columns * waves % total)
        parts += [np.cos(angle), np.sin(angle)]
    return np.concatenate(parts, axis=0).astype(np.float32)


class Group:
    def __init__(self, me, count, device):
        self.me, self.count, self.device = me, count, device


class Exchange:
    def __init__(self, group, sems, row, src_of, dst_of):
        self.group, self.sems, self.row = group, sems, row
        self.src_of, self.dst_of = src_of, dst_of

    def copy(self, peer, slot):
        return pltpu.make_async_remote_copy(
            src_ref=self.src_of(peer),
            dst_ref=self.dst_of(slot),
            send_sem=self.sems.at[2 * self.row, peer],
            recv_sem=self.sems.at[2 * self.row + 1, slot],
            device_id=self.group.device(peer),
            device_id_type=MESH,
        )

    def each(self, act):
        group = self.group

        def step(k, carry):
            act(lax.rem(group.me + k, group.count))
            return carry

        lax.fori_loop(1, group.count, step, 0)

    def start(self):
        self.each(lambda peer: self.copy(peer, self.group.me).start())

    def wait_recv(self):
        self.each(lambda peer: self.copy(peer, peer).wait_recv())

    def wait_send(self):
        self.each(lambda peer: self.copy(peer, peer).wait_send())


def meet(*groups):
    barrier = pltpu.get_barrier_semaphore()
    for group in groups:

        def step(k, carry, group=group):
            peer = lax.rem(group.me + k, group.count)
            pl.semaphore_signal(
                barrier, inc=1, device_id=group.device(peer), device_id_type=MESH
            )
            return carry

        lax.fori_loop(1, group.count, step, 0)


def met(*groups):
    pl.semaphore_wait(pltpu.get_barrier_semaphore(), sum(g.count - 1 for g in groups))


def lanes(index):
    return pl.ds(pl.multiple_of(index * WIDE, WIDE), WIDE)


def chunk(index, size=CHUNK):
    return pl.ds(pl.multiple_of(index * size, size), size)


def split(x):
    high = x.astype(BF16)
    return high, (x - high.astype(F32)).astype(BF16)


def mm(a, b, dims):
    return lax.dot_general(a, b, (dims, ((), ())), preferred_element_type=F32)


def mm3(a, b, dims):
    return mm(a[0], b[0], dims) + (mm(a[0], b[1], dims) + mm(a[1], b[0], dims))


def stack(x):
    return jnp.concatenate(split(x), axis=0)


def mm3s(both, b, dims):
    rows = both.shape[0] // 2
    value = mm(both, b[0], dims)
    return value[:rows] + value[rows:] + mm(both[:rows], b[1], dims)


def pair_sums(buffer, into):
    for t in range(SUBS):
        into[t] = buffer[2 * t] + buffer[2 * t + 1]


def suffix_sums(rows, into):
    total = rows[SUBS - 1]
    into[SUBS - 1] = total
    for t in range(SUBS - 2, -1, -1):
        total = total + rows[t]
        into[t] = total


def prefix_sums(rows, into):
    total = rows[0]
    into[0] = total
    for t in range(1, SUBS):
        total = total + rows[t]
        into[t] = total


def lagged_sums(rows, into):
    total = jnp.zeros_like(rows[0])
    for t in range(SUBS):
        into[t] = total
        total = total + rows[t]


def fold(x):
    return jnp.sum(x.reshape(x.shape[0] // 8, 8, x.shape[1]), axis=0)


class Sums:
    def __init__(self):
        self.held = None

    def add(self, x0, x1, x2, scale=None):
        d0, d1 = x0 - x1, x1 - x2
        terms = (d0 * x0, d0 * d0, d0 * x1 + d1 * x0, d1 * x1, d0 * d1, d1 * d1)
        terms = [fold(x) for x in terms]
        if scale is not None:
            terms = [x * scale for x in terms]
        self.held = terms if self.held is None else [a + b for a, b in zip(self.held, terms)]

    def tile(self):
        rows = [jnp.sum(x, axis=0, keepdims=True) for x in self.held]
        return jnp.concatenate(rows + [jnp.zeros((1, WIDE), F32)] * 2, axis=0)


INPUTS = (
    "b", "obs", "l0", "traj", "w_in", "w_out", "modes", "base", "scale", "limit", "ocol", "count",
    "vrow",
)
OUTPUTS = ("mult", "obs_a", "obs_b", "incr_a", "incr_b")
NAMES = (
    "shift", "vpair", "vz", "vcore", "hl", "hb", "hr", "nfw", "mret", "sret", "mful", "efw",
    "m2ret", "tfw", "qret", "m2ful", "afw", "ufw", "gat1", "gat2", "red1", "amp0", "lba", "amp1",
    "bak1", "amp2", "bak2", "red2", "clx",
)


def scratch_list(deep, width, hidden, total_cols):
    piece = deep // RING
    field, every = (RING, piece, width), (SUBS, piece, width)
    amps, flat = (COLN, PAD, width), (PAD, total_cols)
    coef, wide = (RING, PAD, 2 * KW), (GRPS, PAD, total_cols)
    back = (COLN, GRPS, PAD, width)
    out = {
        "fin": ((hidden, deep), F32), "fout": ((deep, hidden), F32),
        "wih": ((hidden, deep), BF16), "wil": ((hidden, deep), BF16),
        "woh": ((deep, hidden), BF16), "wol": ((deep, hidden), BF16),
        "slp": ((width, hidden), F32), "hh": ((2 * width, hidden), BF16),
        "zz": ((2 * width, deep), BF16), "ot": ((width, deep), F32),
        "vpad": ((COLN, PAD, deep), F32), "voth": ((COLN // CORES, CORES, PAD, deep), F32),
        "vah": ((GRPS, COLN * PAD, deep), BF16), "val": ((GRPS, COLN * PAD, deep), BF16),
        "seen": ((64, deep), F32), "seen2": ((64, deep), F32), "p3t": ((width, deep), F32),
        "ht": ((width, deep), F32), "qt": ((width, deep), F32),
        "cl": ((GRPS, PAD, 2 * KW), F32),
        "thi": ((total_cols, 2 * KW), BF16), "tlo": ((total_cols, 2 * KW), BF16),
        "spec": ((PAD, 2 * KW), F32), "var": ((64, 1), F32), "fmod": ((deep // GRPS, deep), F32),
        "pick": ((width, 64), BF16), "pick_t": ((64, width), BF16),
        "r1": (field, F32), "p3": (field, F32), "q": (field, F32),
        "rb1": ((RING, 8, WIDE), F32), "rb2": ((COLN, 8, WIDE), F32),
    }
    for name in ("lup", "np_", "nbuf", "mup", "sb", "mfull", "ep", "ebuf", "m2up", "tp", "tbuf",
                 "qs", "m2full", "ap", "abuf", "up", "ubuf"):
        out[name] = (field, F32)
    for name in ("nt", "mt", "bt", "sbt", "l0t", "r1t", "et", "m2t", "t1t", "qst"):
        out[name] = (every, F32)
    for i in range(3):
        out[f"am{i}"] = (amps, F32)
        out[f"cb{i}"] = (flat, F32)
        out[f"wd{i}"] = (wide, F32)
        out[f"bk{i}"] = (back, F32)
    for i in (1, 2):
        out[f"gb{i}"] = (coef, F32)
    return out


def kernel(names, *refs):
    x = types.SimpleNamespace(**dict(zip(names, refs)))
    s, c, g = lax.axis_index("sub"), lax.axis_index("col"), lax.axis_index("grp")
    core, z = lax.rem(c, CORES), lax.div(c, CORES)
    r = s * GRPS + g
    deep, hidden, width = x.woh.shape[0], x.woh.shape[1], x.slp.shape[0]
    ring = Group(r, RING, lambda p: {"sub": lax.div(p, GRPS), "grp": lax.rem(p, GRPS)})
    subs = Group(s, SUBS, lambda p: {"sub": p})
    cols = Group(c, COLN, lambda p: {"col": p})
    pair = Group(g, GRPS, lambda p: {"grp": p})
    same = Group(z, COLN // CORES, lambda p: {"col": p * CORES + core})
    chip = Group(core, CORES, lambda p: {"col": z * CORES + p})

    def over(name, group, src, dst):
        return Exchange(group, x.sems, NAMES.index(name), src, dst)

    def next_sub(p):
        return lax.rem(lax.div(p, GRPS) + 1, SUBS)

    def forward(name, src, dst):
        return over(name, ring, lambda p: src.at[p], lambda i: dst.at[i])

    def giving(name, src, dst):
        return over(name, ring, lambda p: src.at[lax.div(p, GRPS)], lambda i: dst.at[i])

    def giving_next(name, src, dst):
        return over(name, ring, lambda p: src.at[next_sub(p)], lambda i: dst.at[i])

    def halves(name, src, dst):
        return over(name, subs, lambda p: src.at[p * GRPS + g], lambda i: dst.at[i])

    def amps(name, src, dst):
        return over(name, cols, lambda p: src.at[p], lambda i: dst.at[:, lanes(i)])

    def backs(name, src, dst):
        return over(name, cols, lambda p: src.at[:, :, lanes(p)], lambda i: dst.at[i])

    def gathers(name, buf):
        return over(name, ring, lambda p: buf.at[r], lambda i: buf.at[i])

    row = NAMES.index("shift")
    shift = pltpu.make_async_remote_copy(
        src_ref=x.l0, dst_ref=x.lup, send_sem=x.sems.at[2 * row, 0],
        recv_sem=x.sems.at[2 * row + 1, 0],
        device_id={"sub": lax.rem(s + SUBS - 1, SUBS)}, device_id_type=MESH,
    )
    vpair = over("vpair", pair, lambda p: x.vpad.at[c], lambda i: x.voth.at[z, core])
    vz = over("vz", same, lambda p: x.voth.at[z, core], lambda i: x.voth.at[i, core])
    vcore = over("vcore", chip, lambda p: x.voth.at[:, core], lambda i: x.voth.at[:, i])
    hl = halves("hl", x.l0, x.l0t)
    hb = halves("hb", x.b, x.bt)
    hr = halves("hr", x.r1, x.r1t)
    nfw = forward("nfw", x.np_, x.nbuf)
    mret = giving_next("mret", x.mt, x.mup)
    sret = giving("sret", x.sbt, x.sb)
    mful = giving("mful", x.mt, x.mfull)
    efw = forward("efw", x.ep, x.ebuf)
    m2ret = giving_next("m2ret", x.m2t, x.m2up)
    tfw = forward("tfw", x.tp, x.tbuf)
    qret = giving("qret", x.qst, x.qs)
    m2ful = giving("m2ful", x.m2t, x.m2full)
    afw = forward("afw", x.ap, x.abuf)
    ufw = forward("ufw", x.up, x.ubuf)
    gat1, gat2 = gathers("gat1", x.gb1), gathers("gat2", x.gb2)
    red1 = gathers("red1", x.rb1)
    red2 = over("red2", cols, lambda p: x.rb2.at[c], lambda i: x.rb2.at[i])
    amp0, amp1, amp2 = (amps(f"amp{i}", getattr(x, f"am{i}"), getattr(x, f"cb{i}")) for i in range(3))
    lba, bak1, bak2 = (
        backs(n, getattr(x, f"wd{i}"), getattr(x, f"bk{i}"))
        for i, n in enumerate(("lba", "bak1", "bak2"))
    )
    clx = over("clx", pair, lambda p: x.cl.at[g], lambda i: x.cl.at[i])
    sent = [vpair, vz, vcore, hl, hb, hr, nfw, mret, sret, mful, efw, m2ret, tfw, qret, m2ful,
            afw, ufw, gat1, gat2, red1, red2, amp0, amp1, amp2, lba, bak1, bak2, clx]

    get_in = pltpu.make_async_copy(x.w_in, x.fin, x.local.at[0])
    get_out = pltpu.make_async_copy(x.w_out, x.fout, x.local.at[1])
    get_in.start()
    get_modes = pltpu.make_async_copy(x.modes, x.fmod, x.local.at[2])
    get_out.start()
    get_modes.start()

    def first_half(columns):
        weights = (x.woh, x.wol) if columns else (x.wih, x.wil)

        def step(j, carry):
            at = (slice(None), chunk(j)) if columns else (chunk(j), slice(None))
            pair_ = (weights[0][at], weights[1][at])
            value = mm3s(x.zz[...], pair_, ROWS if columns else BACK)
            x.hh[:, chunk(j)] = stack(value * x.slp[:, chunk(j)])
            return carry

        lax.fori_loop(0, hidden // CHUNK, step, 0)

    def second_half(columns):
        weights = (x.wih, x.wil) if columns else (x.woh, x.wol)

        def part(at):
            where = (slice(None), at) if columns else (at, slice(None))
            pair_ = (weights[0][where], weights[1][where])
            x.ot[:, at] = mm3s(x.hh[...], pair_, ROWS if columns else BACK)

        def step(j, carry):
            part(chunk(j))
            return carry

        lax.fori_loop(0, deep // CHUNK, step, 0)
        left = deep % CHUNK
        if left:
            part(pl.ds(deep - left, left))

    def adjoint(zt):
        x.zz[...] = stack(zt)
        first_half(True)
        second_half(True)
        return x.ot[...]

    def tangent(zt, between=lambda: None):
        x.zz[...] = stack(zt)
        first_half(False)
        between()
        second_half(False)
        return x.ot[...]

    def whole(ref):
        return ref[...].reshape(deep, width)

    def put(ref, value_t):
        ref[...] = value_t.T.reshape(ref.shape)

    def amplitudes(ref, into):
        high, low = split(whole(ref))
        value = mm(x.vah[g], jnp.concatenate([high, low], axis=1), ROWS)
        value = value[:, :width] + value[:, width:] + mm(x.val[g], high, ROWS)
        into[...] = value.reshape(into.shape)

    def restored_t(bk):
        total = None
        for h in range(GRPS):
            turned = stack(bk[:, h].reshape(COLN * PAD, width).T)
            term = mm3s(turned, (x.vah[h], x.val[h]), ROWS)
            total = term if total is None else total + term
        return total

    def coefficients(cb):
        return mm3(split(cb[...]), (x.thi[...], x.tlo[...]), ROWS) * x.spec[...]

    def spread_back(values, into):
        value = mm3s(stack(values), (x.thi[...], x.tlo[...]), BACK)
        into[...] = value.reshape(into.shape)

    def summed(gb):
        parts = []
        for h in range(GRPS):
            total = gb[GRPS * (SUBS - 1) + h]
            for u in range(SUBS - 1):
                total = total + jnp.where(u + 1 <= s, 1.0, 0.0) * gb[GRPS * u + h]
            parts.append(total)
        return jnp.concatenate(parts, axis=0)

    def pick_rows(vt):
        high, low = split(vt)
        return mm(x.pick_t[...], high, ROWS) + mm(x.pick_t[...], low, ROWS)

    def spread_rows(values):
        high, low = split(values)
        return mm(x.pick[...], high, ROWS) + mm(x.pick[...], low, ROWS)

    has_later = jnp.where(s < SUBS - 1, 1.0, 0.0)
    leads = jnp.where(g == 0, 1.0, 0.0)

    owned = x.modes.shape[0] // COLN
    meet(ring, cols)
    traj_t = x.traj[...].astype(F32).T
    x.zz[:width] = traj_t.astype(BF16)
    met(ring, cols)
    shift.start()
    hb.start()
    x.bt[s] = x.b[r]
    x.l0t[s] = x.l0[r]
    get_in.wait()

    def open_in(j, carry):
        high, low = split(x.fin[chunk(j), :])
        x.wih[chunk(j), :] = high
        x.wil[chunk(j), :] = low
        inner = mm(x.zz[:width], high, BACK) + mm(x.zz[:width], low, BACK)
        x.slp[:, chunk(j)] = 1.0 - jnp.tanh(inner) ** 2
        return carry

    lax.fori_loop(0, hidden // CHUNK, open_in, 0)
    get_out.wait()

    def open_out(j, carry):
        high, low = split(x.fout[chunk(j, 64), :])
        x.woh[chunk(j, 64), :] = high
        x.wol[chunk(j, 64), :] = low
        return carry

    lax.fori_loop(0, deep // 64, open_out, 0)
    shift.wait_recv()
    put(x.np_, adjoint(whole(x.lup).T) * has_later)
    nfw.start()
    x.nbuf[r] = x.np_[r]
    get_modes.wait()
    for i in range(COLN):
        x.vpad[i, :owned] = x.fmod[i * owned:(i + 1) * owned]
        x.vpad[i, owned:] = jnp.zeros((PAD - owned, deep), F32)
    vpair.start()
    high, low = split(x.vpad[...].reshape(COLN * PAD, deep))
    x.vah[g] = high
    x.val[g] = low
    amplitudes(x.l0, x.am0)
    amp0.start()
    x.cb0[:, lanes(c)] = x.am0[c]

    def iota(shape, dim):
        return lax.broadcasted_iota(jnp.int32, shape, dim)

    total_cols = width * COLN
    first_mode = g * (owned * COLN) + c * owned
    scales = limits = jnp.zeros((PAD, WIDE), F32)
    for q in range(deep // WIDE):
        own = iota((PAD, WIDE), 1) + q * WIDE == iota((PAD, WIDE), 0) + first_mode
        scales = scales + jnp.where(own, x.scale[q:q + 1, :], 0.0)
        limits = limits + jnp.where(own, x.limit[q:q + 1, :].astype(F32), 0.0)
    scales = jnp.sum(scales, axis=1, keepdims=True)
    limits = jnp.sum(limits, axis=1, keepdims=True)
    wave = iota((PAD, KW), 1).astype(F32)
    decay = jnp.exp(-0.5 * (2.0 * math.pi * wave * scales / total_cols) ** 2)
    factor = jnp.where(iota((PAD, KW), 1) == 0, 1.0, 2.0) / total_cols
    values = decay * factor * jnp.where(wave < limits, 1.0, 0.0)
    x.spec[:, :KW] = values
    x.spec[:, KW:] = values
    slots = x.obs.shape[0]
    chosen = jnp.where(iota((1, slots), 1) < x.count[...], x.ocol[...] - c * width, -1)
    chosen = chosen.astype(F32)
    eye = iota((slots, slots), 0) == iota((slots, slots), 1)
    down = jnp.sum(jnp.where(eye, chosen, 0.0), axis=1, keepdims=True)
    x.var[...] = jnp.sum(jnp.where(eye, x.vrow[...], 0.0), axis=1, keepdims=True)
    near = iota((width, slots), 0).astype(F32) == chosen
    x.pick[...] = jnp.where(near, 1.0, 0.0).astype(BF16)
    near = iota((slots, width), 1).astype(F32) == down
    x.pick_t[...] = jnp.where(near, 1.0, 0.0).astype(BF16)

    def open_table(p, carry):
        cos_in, sin_in = x.base[:WIDE], x.base[WIDE:2 * WIDE]
        cos_at = x.base[pl.ds(2 * WIDE + p, 1)]
        sin_at = x.base[pl.ds(2 * WIDE + COLN + p, 1)]
        rows = chunk(p, WIDE)
        high, low = split(cos_at * cos_in - sin_at * sin_in)
        x.thi[rows, :KW], x.tlo[rows, :KW] = high, low
        high, low = split(sin_at * cos_in + cos_at * sin_in)
        x.thi[rows, KW:], x.tlo[rows, KW:] = high, low
        return carry

    lax.fori_loop(0, COLN, open_table, 0)
    vpair.wait_recv()
    vz.start()
    x.ht[...] = spread_rows(x.obs[...] / x.var[...])
    nfw.wait_recv()
    pair_sums(x.nbuf, x.nt)
    suffix_sums(x.nt, x.mt)
    mret.start()
    x.mup[r] = x.mt[lax.rem(s + 1, SUBS)]
    hb.wait_recv()
    prefix_sums(x.bt, x.sbt)
    sret.start()
    x.sb[r] = x.sbt[s]
    mful.start()
    x.mfull[r] = x.mt[s]
    amp0.wait_recv()
    x.cl[g] = coefficients(x.cb0)
    mret.wait_recv()
    amplitudes(x.mup, x.am1)
    amp1.start()
    clx.start()
    x.cb1[:, lanes(c)] = x.am1[c]
    vz.wait_recv()
    vcore.start()
    put(x.ep, adjoint((whole(x.mup) - whole(x.lup)).T) * has_later - leads * x.ht[...])
    amp1.wait_recv()
    x.gb1[r] = coefficients(x.cb1)
    gat1.start()
    efw.start()
    x.ebuf[r] = x.ep[r]
    clx.wait_recv()
    spread_back(x.cl[...].reshape(GRPS * PAD, 2 * KW), x.wd0)
    vcore.wait_recv()
    high, low = split(x.voth[...].reshape(COLN * PAD, deep))
    x.vah[1 - g] = high
    x.val[1 - g] = low
    gat1.wait_recv()
    spread_back(summed(x.gb1), x.wd1)
    bak1.start()
    x.bk1[c] = x.wd1[:, :, lanes(c)]
    efw.wait_recv()
    pair_sums(x.ebuf, x.et)
    suffix_sums(x.et, x.m2t)
    m2ret.start()
    m2ful.start()
    x.m2full[r] = x.m2t[s]
    x.m2up[r] = x.m2t[lax.rem(s + 1, SUBS)]
    m2ret.wait_recv()
    amplitudes(x.m2up, x.am2)
    amp2.start()
    lba.start()
    x.cb2[:, lanes(c)] = x.am2[c]
    x.bk0[c] = x.wd0[:, :, lanes(c)]
    sret.wait_recv()
    bak1.wait_recv()
    p3t = whole(x.sb).T - restored_t(x.bk1)
    x.p3t[...] = p3t

    def between():
        amp2.wait_recv()
        x.gb2[r] = coefficients(x.cb2)
        gat2.start()

    put(x.tp, tangent(p3t, between))
    tfw.start()
    x.tbuf[r] = x.tp[r]
    gat2.wait_recv()
    spread_back(summed(x.gb2), x.wd2)
    bak2.start()
    x.bk2[c] = x.wd2[:, :, lanes(c)]
    put(x.p3, x.p3t[...])
    x.seen[...] = pick_rows(x.p3t[...])
    tfw.wait_recv()
    pair_sums(x.tbuf, x.t1t)
    lagged_sums(x.t1t, x.qst)
    qret.start()
    x.qs[r] = x.qst[s]
    a2 = adjoint(whole(x.m2up).T) * has_later
    put(x.ap, a2 + leads * spread_rows(x.seen[...] / x.var[...]))
    afw.start()
    x.abuf[r] = x.ap[r]
    lba.wait_recv()
    x.r1[...] = x.b[...] - restored_t(x.bk0).T.reshape(x.r1.shape)
    hr.start()
    hl.start()
    x.r1t[s] = x.r1[r]
    qret.wait_recv()
    bak2.wait_recv()
    qt = whole(x.qs).T - restored_t(x.bk2)
    x.qt[...] = qt
    put(x.up, tangent(qt))
    ufw.start()
    x.ubuf[r] = x.up[r]
    put(x.q, x.qt[...])
    x.seen2[...] = pick_rows(x.qt[...])
    sums = Sums()
    for i in range(deep // WIDE):
        at = slice(i * WIDE, (i + 1) * WIDE)
        sums.add(x.obs[:, at], -x.seen[:, at], -x.seen2[:, at], leads)
    hl.wait_recv()
    afw.wait_recv()
    blank = jnp.zeros_like(x.mt[0])
    for t in range(SUBS):
        here = x.mt[t] - x.l0t[t]
        later = x.mt[t + 1] - x.l0t[t + 1] if t < SUBS - 1 else blank
        sums.add(here - later, x.et[t], x.abuf[2 * t] + x.abuf[2 * t + 1])
    hr.wait_recv()
    ufw.wait_recv()
    for t in range(SUBS):
        x1 = x.t1t[t - 1] if t else blank
        x2 = x.ubuf[2 * t - 2] + x.ubuf[2 * t - 1] if t else blank
        sums.add(x.r1t[t], x1, x2)
    x.rb1[r] = sums.tile()
    red1.start()
    red1.wait_recv()
    total = x.rb1[0]
    for i in range(1, RING):
        total = total + x.rb1[i]
    x.rb2[c] = total
    red2.start()
    mful.wait_recv()
    m2ful.wait_recv()
    red2.wait_recv()
    total = x.rb2[0]
    for i in range(1, COLN):
        total = total + x.rb2[i]
    gram = jnp.sum(total, axis=1, keepdims=True)
    gram = [gram[i:i + 1] for i in range(6)]
    a = gram[0] / gram[1]
    b = 1.0 - a
    upper = b * b * gram[0] + a * b * gram[2] + a * a * gram[3]
    lower = b * b * gram[1] + 2.0 * a * b * gram[4] + a * a * gram[5]
    a_next = upper / lower
    one, two = a + a_next * b, a_next * a
    move = whole(x.mfull) - whole(x.l0)
    x.mult[...] = (one * move + two * whole(x.m2full)).reshape(x.mult.shape)
    x.incr_a[...] = (one * whole(x.p3)).reshape(x.incr_a.shape)
    x.incr_b[...] = (two * whole(x.q)).reshape(x.incr_b.shape)
    x.obs_a[...] = one * (x.obs[...] / x.var[...])
    x.obs_b[...] = two * (x.seen[...] / x.var[...])
    for one in sent:
        one.wait_send()
    shift.wait_send()


def on_device(
    first_rhs,
    innovations,
    start_mult,
    trajectory,
    weight_in,
    weight_out,
    vertical_modes,
    length_scale,
    band_limit,
    obs_col,
    obs_count,
    obs_var,
):
    deep, width = first_rhs.shape[1:]
    slots = innovations.shape[1]
    hidden = weight_in.shape[0]
    total_cols = width * COLN
    field = (RING, deep // RING, width)

    vmem = pl.BlockSpec(memory_space=pltpu.VMEM)
    away = pl.BlockSpec(memory_space=pl.ANY)
    args = dict(
        b=first_rhs.reshape(field), obs=innovations[0], l0=start_mult.reshape(field),
        traj=trajectory[0], w_in=weight_in, w_out=weight_out, modes=vertical_modes,
        base=jnp.asarray(base_tables(total_cols)), scale=length_scale.reshape(-1, WIDE),
        limit=band_limit.reshape(-1, WIDE), ocol=obs_col, count=obs_count, vrow=obs_var,
    )
    scratch = scratch_list(deep, width, hidden, total_cols)
    names = INPUTS + OUTPUTS + tuple(scratch) + ("local", "sems")
    shapes = (field, (slots, deep), (slots, deep), field, field)
    move, obs_a, obs_b, incr_a, incr_b = pl.pallas_call(
        lambda *refs: kernel(names, *refs),
        name="saddle",
        out_shape=[jax.ShapeDtypeStruct(shape, F32) for shape in shapes],
        in_specs=[away if n in ("w_in", "w_out", "modes") else vmem for n in INPUTS],
        out_specs=[vmem] * len(shapes),
        scratch_shapes=[pltpu.VMEM(*scratch[n]) for n in scratch]
        + [pltpu.SemaphoreType.DMA((3,)), pltpu.SemaphoreType.DMA((2 * len(NAMES), 16))],
        compiler_params=pltpu.CompilerParams(collective_id=0, has_side_effects=True),
    )(*(args[n] for n in INPUTS))
    mult = start_mult + move.reshape(1, deep, width)
    incr = incr_a + incr_b
    return mult, (obs_a - obs_b)[None], incr.reshape(1, deep, width)


def solution(mesh):
    in_specs = (
        P("sub", None, "col"),
        P("sub", "col", None),
        P("sub", None, "col"),
        P("sub", None, "col"),
        P("grp", None),
        P(None, "grp"),
        P("grp", None),
        P(),
        P(),
        P("sub", "col"),
        P("sub", "col"),
        P("sub", "col"),
    )
    out_specs = (P("sub", None, "col"), P("sub", "col", None), P("sub", None, "col"))
    return jax.shard_map(
        on_device, mesh=mesh, in_specs=in_specs, out_specs=out_specs, check_vma=False
    )
```

```python
import math
import types

import jax
import jax.numpy as jnp
import numpy as np
from jax import lax
from jax.experimental import pallas as pl
from jax.experimental.pallas import tpu as pltpu
from jax.sharding import PartitionSpec as P

KW = 128
SUBS = 8
COLN = 16
GRPS = 2
CORES = 2
RING = SUBS * GRPS
PAD = 24
WIDE = 128
CHUNK = 256
STRIP = 64
MESH = pl.DeviceIdType.MESH
F32 = jnp.float32
BF16 = jnp.bfloat16
ROWS = ((1,), (0,))
BACK = ((1,), (1,))


def base_tables(total):
    waves = np.arange(KW)[None, :]
    inner, outer = np.arange(WIDE)[:, None], np.arange(0, total, WIDE)[:, None]
    parts = []
    for columns in (inner, outer):
        angle = 2.0 * math.pi / total * (columns * waves % total)
        parts += [np.cos(angle), np.sin(angle)]
    return np.concatenate(parts, axis=0).astype(np.float32)


class Group:
    def __init__(self, me, count, device):
        self.me, self.count, self.device = me, count, device


class Exchange:
    def __init__(self, group, sems, row, src_of, dst_of, all_ref):
        self.group, self.sems, self.row = group, sems, row
        self.src_of, self.dst_of, self.all_ref = src_of, dst_of, all_ref

    def copy(self, src, dst, peer):
        return pltpu.make_async_remote_copy(
            src_ref=src,
            dst_ref=dst,
            send_sem=self.sems.at[2 * self.row],
            recv_sem=self.sems.at[2 * self.row + 1],
            device_id=self.group.device(peer),
            device_id_type=MESH,
        )

    def start(self):
        group = self.group

        def step(k, carry):
            peer = lax.rem(group.me + k, group.count)
            self.copy(self.src_of(peer), self.dst_of(group.me), peer).start()
            return carry

        lax.fori_loop(1, group.count, step, 0)

    def whole(self):
        peer = lax.rem(self.group.me + 1, self.group.count)
        return self.copy(self.all_ref, self.all_ref, peer)

    def wait_recv(self):
        self.whole().wait_recv()

    def wait_send(self):
        self.whole().wait_send()


def meet(*groups):
    barrier = pltpu.get_barrier_semaphore()
    for group in groups:

        def step(k, carry, group=group):
            peer = lax.rem(group.me + k, group.count)
            pl.semaphore_signal(
                barrier, inc=1, device_id=group.device(peer), device_id_type=MESH
            )
            return carry

        lax.fori_loop(1, group.count, step, 0)


def met(*groups):
    pl.semaphore_wait(pltpu.get_barrier_semaphore(), sum(g.count - 1 for g in groups))


def lanes(index):
    return pl.ds(pl.multiple_of(index * WIDE, WIDE), WIDE)


def chunk(index, size=CHUNK):
    return pl.ds(pl.multiple_of(index * size, size), size)


def split(x):
    high = x.astype(BF16)
    return high, (x - high.astype(F32)).astype(BF16)


def mm(a, b, dims):
    return lax.dot_general(a, b, (dims, ((), ())), preferred_element_type=F32)


def mm3(a, b, dims):
    return mm(a[0], b[0], dims) + (mm(a[0], b[1], dims) + mm(a[1], b[0], dims))


def stack(x):
    return jnp.concatenate(split(x), axis=0)


def mm3s(both, b, dims):
    rows = both.shape[0] // 2
    value = mm(both, b[0], dims)
    return value[:rows] + value[rows:] + mm(both[:rows], b[1], dims)


def pair_sums(buffer, into):
    for t in range(SUBS):
        into[t] = buffer[2 * t] + buffer[2 * t + 1]


def suffix_sums(rows, into):
    total = rows[SUBS - 1]
    into[SUBS - 1] = total
    for t in range(SUBS - 2, -1, -1):
        total = total + rows[t]
        into[t] = total


def prefix_sums(rows, into):
    total = rows[0]
    into[0] = total
    for t in range(1, SUBS):
        total = total + rows[t]
        into[t] = total


def lagged_sums(rows, into):
    total = jnp.zeros_like(rows[0])
    for t in range(SUBS):
        into[t] = total
        total = total + rows[t]


def fold(x):
    return jnp.sum(x.reshape(x.shape[0] // 8, 8, x.shape[1]), axis=0)


class Sums:
    def __init__(self):
        self.held = None

    def add(self, x0, x1, x2, scale=None):
        d0, d1 = x0 - x1, x1 - x2
        terms = (d0 * x0, d0 * d0, d0 * x1 + d1 * x0, d1 * x1, d0 * d1, d1 * d1)
        terms = [fold(x) for x in terms]
        if scale is not None:
            terms = [x * scale for x in terms]
        self.held = terms if self.held is None else [a + b for a, b in zip(self.held, terms)]

    def tile(self):
        rows = [jnp.sum(x, axis=0, keepdims=True) for x in self.held]
        return jnp.concatenate(rows + [jnp.zeros((1, WIDE), F32)] * 2, axis=0)


INPUTS = (
    "b", "obs", "l0", "traj", "w_in", "w_out", "modes", "base", "scale", "limit", "ocol", "count",
    "vrow",
)
LOADS = {
    "l0": "l0", "traj": "traj", "b": "b", "modes": "fmod", "obs": "obs", "base": "base",
    "scale": "scale", "limit": "limit", "ocol": "ocol", "count": "count", "vrow": "vrow",
}
OUTPUTS = ("mult", "obs_a", "obs_b", "incr_a", "incr_b")
NAMES = (
    "shift", "vpair", "vz", "vcore", "hl", "hb", "hr", "nfw", "mret", "sret", "mful", "efw",
    "m2ret", "tfw", "qret", "m2ful", "afw", "ufw", "gat1", "gat2", "red1", "amp0", "lba", "amp1",
    "bak1", "amp2", "bak2", "red2", "clx",
)


def scratch_list(deep, width, hidden, total_cols):
    piece = deep // RING
    field, every = (RING, piece, width), (SUBS, piece, width)
    amps, flat = (COLN, PAD, width), (PAD, total_cols)
    coef, wide = (RING, PAD, 2 * KW), (GRPS, PAD, total_cols)
    back = (COLN, GRPS, PAD, width)
    out = {
        "fin": ((hidden, deep), F32), "fout": ((deep, hidden), F32),
        "wih": ((hidden, deep), BF16), "wil": ((hidden, deep), BF16),
        "woh": ((deep, hidden), BF16), "wol": ((deep, hidden), BF16),
        "slp": ((width, hidden), F32), "hh": ((2 * width, hidden), BF16),
        "zz": ((2 * width, deep), BF16), "ot": ((width, deep), F32),
        "vpad": ((COLN, PAD, deep), F32), "voth": ((COLN // CORES, CORES, PAD, deep), F32),
        "vah": ((GRPS, COLN * PAD, deep), BF16), "val": ((GRPS, COLN * PAD, deep), BF16),
        "seen": ((64, deep), F32), "seen2": ((64, deep), F32), "p3t": ((width, deep), F32),
        "ht": ((width, deep), F32), "qt": ((width, deep), F32),
        "cl": ((GRPS, PAD, 2 * KW), F32),
        "thi": ((total_cols, 2 * KW), BF16), "tlo": ((total_cols, 2 * KW), BF16),
        "spec": ((PAD, 2 * KW), F32), "var": ((64, 1), F32),
        "pick": ((width, 64), BF16), "pick_t": ((64, width), BF16),
        "r1": (field, F32), "p3": (field, F32), "q": (field, F32),
        "rb1": ((RING, 8, WIDE), F32), "rb2": ((COLN, 8, WIDE), F32),
    }
    for name in ("lup", "np_", "nbuf", "mup", "sb", "mfull", "ep", "ebuf", "m2up", "tp", "tbuf",
                 "qs", "m2full", "ap", "abuf", "up", "ubuf"):
        out[name] = (field, F32)
    for name in ("nt", "mt", "bt", "sbt", "l0t", "r1t", "et", "m2t", "t1t", "qst"):
        out[name] = (every, F32)
    loaded = {
        "b": (field, F32), "obs": ((64, deep), F32), "l0": (field, F32),
        "traj": ((deep, width), BF16), "fmod": ((deep // GRPS, deep), F32),
        "base": ((2 * WIDE + 2 * COLN, KW), F32), "scale": ((deep // WIDE, WIDE), F32),
        "limit": ((deep // WIDE, WIDE), jnp.int32), "ocol": ((1, 64), jnp.int32),
        "count": ((1, 1), jnp.int32), "vrow": ((1, 64), F32),
    }
    for name, kind in loaded.items():
        out["in_" + name] = kind
    for i in range(3):
        out[f"am{i}"] = (amps, F32)
        out[f"cb{i}"] = (flat, F32)
        out[f"wd{i}"] = (wide, F32)
        out[f"bk{i}"] = (back, F32)
    for i in (1, 2):
        out[f"gb{i}"] = (coef, F32)
    return out


def kernel(names, *refs):
    given = dict(zip(names, refs))
    loads = {n: (given[n], given["in_" + to]) for n, to in LOADS.items()}
    x = types.SimpleNamespace(**given)
    for n, to in LOADS.items():
        setattr(x, to, given["in_" + to])
    s, c, g = lax.axis_index("sub"), lax.axis_index("col"), lax.axis_index("grp")
    core, z = lax.rem(c, CORES), lax.div(c, CORES)
    r = s * GRPS + g
    deep, hidden, width = x.woh.shape[0], x.woh.shape[1], x.slp.shape[0]
    ring = Group(r, RING, lambda p: {"sub": lax.div(p, GRPS), "grp": lax.rem(p, GRPS)})
    subs = Group(s, SUBS, lambda p: {"sub": p})
    cols = Group(c, COLN, lambda p: {"col": p})
    pair = Group(g, GRPS, lambda p: {"grp": p})
    same = Group(z, COLN // CORES, lambda p: {"col": p * CORES + core})
    chip = Group(core, CORES, lambda p: {"col": z * CORES + p})

    def over(name, group, src, dst, all_ref):
        return Exchange(group, x.sems, NAMES.index(name), src, dst, all_ref)

    def others(ref, group):
        return ref.at[pl.ds(0, group.count - 1)]

    def next_sub(p):
        return lax.rem(lax.div(p, GRPS) + 1, SUBS)

    def forward(name, src, dst):
        return over(name, ring, lambda p: src.at[p], lambda i: dst.at[i], others(dst, ring))

    def giving(name, src, dst):
        at = others(dst, ring)
        return over(name, ring, lambda p: src.at[lax.div(p, GRPS)], lambda i: dst.at[i], at)

    def giving_next(name, src, dst):
        return over(name, ring, lambda p: src.at[next_sub(p)], lambda i: dst.at[i], others(dst, ring))

    def halves(name, src, dst):
        at = others(dst, subs)
        return over(name, subs, lambda p: src.at[p * GRPS + g], lambda i: dst.at[i], at)

    def amps(name, src, dst):
        at = dst.at[:, pl.ds(0, (COLN - 1) * WIDE)]
        return over(name, cols, lambda p: src.at[p], lambda i: dst.at[:, lanes(i)], at)

    def backs(name, src, dst):
        at = others(dst, cols)
        return over(name, cols, lambda p: src.at[:, :, lanes(p)], lambda i: dst.at[i], at)

    def gathers(name, buf):
        return over(name, ring, lambda p: buf.at[r], lambda i: buf.at[i], others(buf, ring))

    row = NAMES.index("shift")
    shift = pltpu.make_async_remote_copy(
        src_ref=x.l0, dst_ref=x.lup, send_sem=x.sems.at[2 * row],
        recv_sem=x.sems.at[2 * row + 1],
        device_id={"sub": lax.rem(s + SUBS - 1, SUBS)}, device_id_type=MESH,
    )
    vpair = over("vpair", pair, lambda p: x.vpad.at[c], lambda i: x.voth.at[z, core], x.voth.at[z, core])
    at = x.voth.at[pl.ds(0, same.count - 1), core]
    vz = over("vz", same, lambda p: x.voth.at[z, core], lambda i: x.voth.at[i, core], at)
    at = x.voth.at[:, 1 - core]
    vcore = over("vcore", chip, lambda p: x.voth.at[:, core], lambda i: x.voth.at[:, i], at)
    hl = halves("hl", x.l0, x.l0t)
    hb = halves("hb", x.b, x.bt)
    hr = halves("hr", x.r1, x.r1t)
    nfw = forward("nfw", x.np_, x.nbuf)
    mret = giving_next("mret", x.mt, x.mup)
    sret = giving("sret", x.sbt, x.sb)
    mful = giving("mful", x.mt, x.mfull)
    efw = forward("efw", x.ep, x.ebuf)
    m2ret = giving_next("m2ret", x.m2t, x.m2up)
    tfw = forward("tfw", x.tp, x.tbuf)
    qret = giving("qret", x.qst, x.qs)
    m2ful = giving("m2ful", x.m2t, x.m2full)
    afw = forward("afw", x.ap, x.abuf)
    ufw = forward("ufw", x.up, x.ubuf)
    gat1, gat2 = gathers("gat1", x.gb1), gathers("gat2", x.gb2)
    red1 = gathers("red1", x.rb1)
    red2 = over("red2", cols, lambda p: x.rb2.at[c], lambda i: x.rb2.at[i], others(x.rb2, cols))
    amp0, amp1, amp2 = (amps(f"amp{i}", getattr(x, f"am{i}"), getattr(x, f"cb{i}")) for i in range(3))
    lba, bak1, bak2 = (
        backs(n, getattr(x, f"wd{i}"), getattr(x, f"bk{i}"))
        for i, n in enumerate(("lba", "bak1", "bak2"))
    )
    clx = over("clx", pair, lambda p: x.cl.at[g], lambda i: x.cl.at[i], x.cl.at[1 - g])
    sent = [vpair, vz, vcore, hl, hb, hr, nfw, mret, sret, mful, efw, m2ret, tfw, qret, m2ful,
            afw, ufw, gat1, gat2, red1, red2, amp0, amp1, amp2, lba, bak1, bak2, clx]

    strips = deep // STRIP

    def get_in(j):
        return pltpu.make_async_copy(x.w_in.at[chunk(j), :], x.fin.at[chunk(j), :], x.local.at[j])

    def get_out(j):
        at = chunk(j, STRIP)
        return pltpu.make_async_copy(x.w_out.at[at, :], x.fout.at[at, :], x.local.at[hidden // CHUNK + j])

    load = {
        n: pltpu.make_async_copy(*loads[n], x.local.at[hidden // CHUNK + strips + i]) for i, n in enumerate(loads)
    }
    for n in ("l0", "traj", "b"):
        load[n].start()
    for j in range(hidden // CHUNK):
        get_in(j).start()
    for j in range(strips):
        get_out(j).start()
    for n in tuple(load)[3:]:
        load[n].start()

    def first_half(columns):
        weights = (x.woh, x.wol) if columns else (x.wih, x.wil)

        def step(j, carry):
            at = (slice(None), chunk(j)) if columns else (chunk(j), slice(None))
            pair_ = (weights[0][at], weights[1][at])
            value = mm3s(x.zz[...], pair_, ROWS if columns else BACK)
            x.hh[:, chunk(j)] = stack(value * x.slp[:, chunk(j)])
            return carry

        lax.fori_loop(0, hidden // CHUNK, step, 0)

    def second_half(columns):
        weights = (x.wih, x.wil) if columns else (x.woh, x.wol)

        def part(at):
            where = (slice(None), at) if columns else (at, slice(None))
            pair_ = (weights[0][where], weights[1][where])
            x.ot[:, at] = mm3s(x.hh[...], pair_, ROWS if columns else BACK)

        def step(j, carry):
            part(chunk(j))
            return carry

        lax.fori_loop(0, deep // CHUNK, step, 0)
        left = deep % CHUNK
        if left:
            part(pl.ds(deep - left, left))

    def adjoint(zt):
        x.zz[...] = stack(zt)
        first_half(True)
        second_half(True)
        return x.ot[...]

    def tangent(zt, between=lambda: None):
        x.zz[...] = stack(zt)
        first_half(False)
        between()
        second_half(False)
        return x.ot[...]

    def whole(ref):
        return ref[...].reshape(deep, width)

    def put(ref, value_t):
        ref[...] = value_t.T.reshape(ref.shape)

    def amplitudes(ref, into):
        high, low = split(whole(ref))
        value = mm(x.vah[g], jnp.concatenate([high, low], axis=1), ROWS)
        value = value[:, :width] + value[:, width:] + mm(x.val[g], high, ROWS)
        into[...] = value.reshape(into.shape)

    def restored_t(bk):
        total = None
        for h in range(GRPS):
            turned = stack(bk[:, h].reshape(COLN * PAD, width).T)
            term = mm3s(turned, (x.vah[h], x.val[h]), ROWS)
            total = term if total is None else total + term
        return total

    def coefficients(cb):
        return mm3(split(cb[...]), (x.thi[...], x.tlo[...]), ROWS) * x.spec[...]

    def spread_back(values, into):
        value = mm3s(stack(values), (x.thi[...], x.tlo[...]), BACK)
        into[...] = value.reshape(into.shape)

    def summed(gb):
        parts = []
        for h in range(GRPS):
            total = gb[GRPS * (SUBS - 1) + h]
            for u in range(SUBS - 1):
                total = total + jnp.where(u + 1 <= s, 1.0, 0.0) * gb[GRPS * u + h]
            parts.append(total)
        return jnp.concatenate(parts, axis=0)

    def pick_rows(vt):
        high, low = split(vt)
        return mm(x.pick_t[...], high, ROWS) + mm(x.pick_t[...], low, ROWS)

    def spread_rows(values):
        high, low = split(values)
        return mm(x.pick[...], high, ROWS) + mm(x.pick[...], low, ROWS)

    has_later = jnp.where(s < SUBS - 1, 1.0, 0.0)
    leads = jnp.where(g == 0, 1.0, 0.0)

    owned = x.fmod.shape[0] // COLN
    meet(ring, cols)
    load["l0"].wait()
    load["traj"].wait()
    traj_t = x.traj[...].astype(F32).T
    x.zz[:width] = traj_t.astype(BF16)
    met(ring, cols)
    shift.start()
    load["b"].wait()
    hb.start()
    x.bt[s] = x.b[r]
    x.l0t[s] = x.l0[r]

    def open_in(j, carry):
        get_in(j).wait()
        high, low = split(x.fin[chunk(j), :])
        x.wih[chunk(j), :] = high
        x.wil[chunk(j), :] = low
        inner = mm(x.zz[:width], high, BACK) + mm(x.zz[:width], low, BACK)
        x.slp[:, chunk(j)] = 1.0 - jnp.tanh(inner) ** 2
        return carry

    lax.fori_loop(0, hidden // CHUNK, open_in, 0)

    def open_out(j, carry):
        get_out(j).wait()
        at = chunk(j, STRIP)
        high, low = split(x.fout[at, :])
        x.woh[at, :] = high
        x.wol[at, :] = low
        return carry

    lax.fori_loop(0, strips, open_out, 0)
    shift.wait_recv()
    put(x.np_, adjoint(whole(x.lup).T) * has_later)
    nfw.start()
    x.nbuf[r] = x.np_[r]
    for n in tuple(load)[3:]:
        load[n].wait()
    for i in range(COLN):
        x.vpad[i, :owned] = x.fmod[i * owned:(i + 1) * owned]
        x.vpad[i, owned:] = jnp.zeros((PAD - owned, deep), F32)
    vpair.start()
    high, low = split(x.vpad[...].reshape(COLN * PAD, deep))
    x.vah[g] = high
    x.val[g] = low
    amplitudes(x.l0, x.am0)
    amp0.start()
    x.cb0[:, lanes(c)] = x.am0[c]

    def iota(shape, dim):
        return lax.broadcasted_iota(jnp.int32, shape, dim)

    total_cols = width * COLN
    first_mode = g * (owned * COLN) + c * owned
    scales = limits = jnp.zeros((PAD, WIDE), F32)
    for q in range(deep // WIDE):
        own = iota((PAD, WIDE), 1) + q * WIDE == iota((PAD, WIDE), 0) + first_mode
        scales = scales + jnp.where(own, x.scale[q:q + 1, :], 0.0)
        limits = limits + jnp.where(own, x.limit[q:q + 1, :].astype(F32), 0.0)
    scales = jnp.sum(scales, axis=1, keepdims=True)
    limits = jnp.sum(limits, axis=1, keepdims=True)
    wave = iota((PAD, KW), 1).astype(F32)
    decay = jnp.exp(-0.5 * (2.0 * math.pi * wave * scales / total_cols) ** 2)
    factor = jnp.where(iota((PAD, KW), 1) == 0, 1.0, 2.0) / total_cols
    values = decay * factor * jnp.where(wave < limits, 1.0, 0.0)
    x.spec[:, :KW] = values
    x.spec[:, KW:] = values
    slots = x.obs.shape[0]
    chosen = jnp.where(iota((1, slots), 1) < x.count[...], x.ocol[...] - c * width, -1)
    chosen = chosen.astype(F32)
    eye = iota((slots, slots), 0) == iota((slots, slots), 1)
    down = jnp.sum(jnp.where(eye, chosen, 0.0), axis=1, keepdims=True)
    x.var[...] = jnp.sum(jnp.where(eye, x.vrow[...], 0.0), axis=1, keepdims=True)
    near = iota((width, slots), 0).astype(F32) == chosen
    x.pick[...] = jnp.where(near, 1.0, 0.0).astype(BF16)
    near = iota((slots, width), 1).astype(F32) == down
    x.pick_t[...] = jnp.where(near, 1.0, 0.0).astype(BF16)

    def open_table(p, carry):
        cos_in, sin_in = x.base[:WIDE], x.base[WIDE:2 * WIDE]
        cos_at = x.base[pl.ds(2 * WIDE + p, 1)]
        sin_at = x.base[pl.ds(2 * WIDE + COLN + p, 1)]
        rows = chunk(p, WIDE)
        high, low = split(cos_at * cos_in - sin_at * sin_in)
        x.thi[rows, :KW], x.tlo[rows, :KW] = high, low
        high, low = split(sin_at * cos_in + cos_at * sin_in)
        x.thi[rows, KW:], x.tlo[rows, KW:] = high, low
        return carry

    lax.fori_loop(0, COLN, open_table, 0)
    vpair.wait_recv()
    vz.start()
    x.ht[...] = spread_rows(x.obs[...] / x.var[...])
    nfw.wait_recv()
    pair_sums(x.nbuf, x.nt)
    suffix_sums(x.nt, x.mt)
    mret.start()
    x.mup[r] = x.mt[lax.rem(s + 1, SUBS)]
    hb.wait_recv()
    prefix_sums(x.bt, x.sbt)
    sret.start()
    x.sb[r] = x.sbt[s]
    mful.start()
    x.mfull[r] = x.mt[s]
    amp0.wait_recv()
    x.cl[g] = coefficients(x.cb0)
    mret.wait_recv()
    amplitudes(x.mup, x.am1)
    amp1.start()
    clx.start()
    x.cb1[:, lanes(c)] = x.am1[c]
    vz.wait_recv()
    vcore.start()
    put(x.ep, adjoint((whole(x.mup) - whole(x.lup)).T) * has_later - leads * x.ht[...])
    amp1.wait_recv()
    x.gb1[r] = coefficients(x.cb1)
    gat1.start()
    efw.start()
    x.ebuf[r] = x.ep[r]
    clx.wait_recv()
    spread_back(x.cl[...].reshape(GRPS * PAD, 2 * KW), x.wd0)
    vcore.wait_recv()
    high, low = split(x.voth[...].reshape(COLN * PAD, deep))
    x.vah[1 - g] = high
    x.val[1 - g] = low
    gat1.wait_recv()
    spread_back(summed(x.gb1), x.wd1)
    bak1.start()
    x.bk1[c] = x.wd1[:, :, lanes(c)]
    efw.wait_recv()
    pair_sums(x.ebuf, x.et)
    suffix_sums(x.et, x.m2t)
    m2ret.start()
    m2ful.start()
    x.m2full[r] = x.m2t[s]
    x.m2up[r] = x.m2t[lax.rem(s + 1, SUBS)]
    m2ret.wait_recv()
    amplitudes(x.m2up, x.am2)
    amp2.start()
    lba.start()
    x.cb2[:, lanes(c)] = x.am2[c]
    x.bk0[c] = x.wd0[:, :, lanes(c)]
    sret.wait_recv()
    bak1.wait_recv()
    p3t = whole(x.sb).T - restored_t(x.bk1)
    x.p3t[...] = p3t

    def between():
        amp2.wait_recv()
        x.gb2[r] = coefficients(x.cb2)
        gat2.start()

    put(x.tp, tangent(p3t, between))
    tfw.start()
    x.tbuf[r] = x.tp[r]
    gat2.wait_recv()
    spread_back(summed(x.gb2), x.wd2)
    bak2.start()
    x.bk2[c] = x.wd2[:, :, lanes(c)]
    put(x.p3, x.p3t[...])
    x.seen[...] = pick_rows(x.p3t[...])
    tfw.wait_recv()
    pair_sums(x.tbuf, x.t1t)
    lagged_sums(x.t1t, x.qst)
    qret.start()
    x.qs[r] = x.qst[s]
    a2 = adjoint(whole(x.m2up).T) * has_later
    put(x.ap, a2 + leads * spread_rows(x.seen[...] / x.var[...]))
    afw.start()
    x.abuf[r] = x.ap[r]
    lba.wait_recv()
    x.r1[...] = x.b[...] - restored_t(x.bk0).T.reshape(x.r1.shape)
    hr.start()
    hl.start()
    x.r1t[s] = x.r1[r]
    qret.wait_recv()
    bak2.wait_recv()
    qt = whole(x.qs).T - restored_t(x.bk2)
    x.qt[...] = qt
    put(x.up, tangent(qt))
    ufw.start()
    x.ubuf[r] = x.up[r]
    put(x.q, x.qt[...])
    x.seen2[...] = pick_rows(x.qt[...])
    sums = Sums()
    for i in range(deep // WIDE):
        at = slice(i * WIDE, (i + 1) * WIDE)
        sums.add(x.obs[:, at], -x.seen[:, at], -x.seen2[:, at], leads)
    hl.wait_recv()
    afw.wait_recv()
    blank = jnp.zeros_like(x.mt[0])
    for t in range(SUBS):
        here = x.mt[t] - x.l0t[t]
        later = x.mt[t + 1] - x.l0t[t + 1] if t < SUBS - 1 else blank
        sums.add(here - later, x.et[t], x.abuf[2 * t] + x.abuf[2 * t + 1])
    hr.wait_recv()
    ufw.wait_recv()
    for t in range(SUBS):
        x1 = x.t1t[t - 1] if t else blank
        x2 = x.ubuf[2 * t - 2] + x.ubuf[2 * t - 1] if t else blank
        sums.add(x.r1t[t], x1, x2)
    x.rb1[r] = sums.tile()
    red1.start()
    red1.wait_recv()
    total = x.rb1[0]
    for i in range(1, RING):
        total = total + x.rb1[i]
    x.rb2[c] = total
    red2.start()
    mful.wait_recv()
    m2ful.wait_recv()
    red2.wait_recv()
    total = x.rb2[0]
    for i in range(1, COLN):
        total = total + x.rb2[i]
    gram = jnp.sum(total, axis=1, keepdims=True)
    gram = [gram[i:i + 1] for i in range(6)]
    a = gram[0] / gram[1]
    b = 1.0 - a
    upper = b * b * gram[0] + a * b * gram[2] + a * a * gram[3]
    lower = b * b * gram[1] + 2.0 * a * b * gram[4] + a * a * gram[5]
    a_next = upper / lower
    one, two = a + a_next * b, a_next * a
    move = whole(x.mfull) - whole(x.l0)
    x.mult[...] = (one * move + two * whole(x.m2full)).reshape(x.mult.shape)
    x.incr_a[...] = (one * whole(x.p3)).reshape(x.incr_a.shape)
    x.incr_b[...] = (two * whole(x.q)).reshape(x.incr_b.shape)
    x.obs_a[...] = one * (x.obs[...] / x.var[...])
    x.obs_b[...] = two * (x.seen[...] / x.var[...])
    for one in sent:
        one.wait_send()
    shift.wait_send()


def on_device(
    first_rhs,
    innovations,
    start_mult,
    trajectory,
    weight_in,
    weight_out,
    vertical_modes,
    length_scale,
    band_limit,
    obs_col,
    obs_count,
    obs_var,
):
    deep, width = first_rhs.shape[1:]
    slots = innovations.shape[1]
    hidden = weight_in.shape[0]
    total_cols = width * COLN
    field = (RING, deep // RING, width)

    vmem = pl.BlockSpec(memory_space=pltpu.VMEM)
    away = pl.BlockSpec(memory_space=pl.ANY)
    args = dict(
        b=first_rhs.reshape(field), obs=innovations[0], l0=start_mult.reshape(field),
        traj=trajectory[0], w_in=weight_in, w_out=weight_out, modes=vertical_modes,
        base=jnp.asarray(base_tables(total_cols)), scale=length_scale.reshape(-1, WIDE),
        limit=band_limit.reshape(-1, WIDE), ocol=obs_col, count=obs_count, vrow=obs_var,
    )
    scratch = scratch_list(deep, width, hidden, total_cols)
    names = INPUTS + OUTPUTS + tuple(scratch) + ("local", "sems")
    shapes = (field, (slots, deep), (slots, deep), field, field)
    move, obs_a, obs_b, incr_a, incr_b = pl.pallas_call(
        lambda *refs: kernel(names, *refs),
        name="saddle",
        out_shape=[pltpu.VMEM(shape, F32) for shape in shapes],
        in_specs=[away] * len(INPUTS),
        out_specs=[vmem] * len(shapes),
        scratch_shapes=[pltpu.VMEM(*scratch[n]) for n in scratch]
        + [
            pltpu.SemaphoreType.DMA((hidden // CHUNK + deep // STRIP + len(LOADS),)),
            pltpu.SemaphoreType.DMA((2 * len(NAMES),)),
        ],
        compiler_params=pltpu.CompilerParams(collective_id=0, has_side_effects=True, vmem_limit_bytes=59_000_000),
    )(*(args[n] for n in INPUTS))
    mult = start_mult + move.reshape(1, deep, width)
    incr = incr_a + incr_b
    return mult, (obs_a - obs_b)[None], incr.reshape(1, deep, width)


def solution(mesh):
    in_specs = (
        P("sub", None, "col"),
        P("sub", "col", None),
        P("sub", None, "col"),
        P("sub", None, "col"),
        P("grp", None),
        P(None, "grp"),
        P("grp", None),
        P(),
        P(),
        P("sub", "col"),
        P("sub", "col"),
        P("sub", "col"),
    )
    out_specs = (P("sub", None, "col"), P("sub", "col", None), P("sub", None, "col"))
    return jax.shard_map(
        on_device, mesh=mesh, in_specs=in_specs, out_specs=out_specs, check_vma=False
    )
```

```python
import math
import types

import jax
import jax.numpy as jnp
import numpy as np
from jax import lax
from jax.experimental import pallas as pl
from jax.experimental.pallas import tpu as pltpu
from jax.sharding import PartitionSpec as P

KW = 128
SUBS = 8
COLN = 16
GRPS = 2
CORES = 2
RING = SUBS * GRPS
PAD = 24
WIDE = 128
CHUNK = 256
STRIP = 64
MESH = pl.DeviceIdType.MESH
F32 = jnp.float32
BF16 = jnp.bfloat16
ROWS = ((1,), (0,))
BACK = ((1,), (1,))


def base_tables(total):
    waves = np.arange(KW)[None, :]
    inner, outer = np.arange(WIDE)[:, None], np.arange(0, total, WIDE)[:, None]
    parts = []
    for columns in (inner, outer):
        angle = 2.0 * math.pi / total * (columns * waves % total)
        parts += [np.cos(angle), np.sin(angle)]
    return np.concatenate(parts, axis=0).astype(np.float32)


class Group:
    def __init__(self, me, count, device):
        self.me, self.count, self.device = me, count, device


class Exchange:
    def __init__(self, group, sems, row, src_of, dst_of, all_ref):
        self.group, self.sems, self.row = group, sems, row
        self.src_of, self.dst_of, self.all_ref = src_of, dst_of, all_ref

    def copy(self, src, dst, peer):
        return pltpu.make_async_remote_copy(
            src_ref=src,
            dst_ref=dst,
            send_sem=self.sems.at[2 * self.row],
            recv_sem=self.sems.at[2 * self.row + 1],
            device_id=self.group.device(peer),
            device_id_type=MESH,
        )

    def start(self):
        group = self.group

        def step(k, carry):
            peer = lax.rem(group.me + k, group.count)
            self.copy(self.src_of(peer), self.dst_of(group.me), peer).start()
            return carry

        lax.fori_loop(1, group.count, step, 0)

    def whole(self):
        peer = lax.rem(self.group.me + 1, self.group.count)
        return self.copy(self.all_ref, self.all_ref, peer)

    def wait_recv(self):
        self.whole().wait_recv()

    def wait_send(self):
        self.whole().wait_send()


def meet(*groups):
    barrier = pltpu.get_barrier_semaphore()
    for group in groups:

        def step(k, carry, group=group):
            peer = lax.rem(group.me + k, group.count)
            pl.semaphore_signal(
                barrier, inc=1, device_id=group.device(peer), device_id_type=MESH
            )
            return carry

        lax.fori_loop(1, group.count, step, 0)


def met(*groups):
    pl.semaphore_wait(pltpu.get_barrier_semaphore(), sum(g.count - 1 for g in groups))


def lanes(index):
    return pl.ds(pl.multiple_of(index * WIDE, WIDE), WIDE)


def chunk(index, size=CHUNK):
    return pl.ds(pl.multiple_of(index * size, size), size)


def split(x):
    high = x.astype(BF16)
    return high, (x - high.astype(F32)).astype(BF16)


def mm(a, b, dims):
    return lax.dot_general(a, b, (dims, ((), ())), preferred_element_type=F32)


def mm3(a, b, dims):
    return mm(a[0], b[0], dims) + (mm(a[0], b[1], dims) + mm(a[1], b[0], dims))


def stack(x):
    return jnp.concatenate(split(x), axis=0)


def mm3s(both, b, dims):
    rows = both.shape[0] // 2
    value = mm(both, b[0], dims)
    return value[:rows] + value[rows:] + mm(both[:rows], b[1], dims)


ALL = slice(None)
PARTS = (slice(0, 24), slice(24, 40))


def pair_sums(buffer, into, rows=ALL):
    for t in range(SUBS):
        into[t, rows] = buffer[2 * t, rows] + buffer[2 * t + 1, rows]


def suffix_sums(terms, into, rows=ALL):
    total = terms[SUBS - 1, rows]
    into[SUBS - 1, rows] = total
    for t in range(SUBS - 2, -1, -1):
        total = total + terms[t, rows]
        into[t, rows] = total


def prefix_sums(terms, into):
    total = terms[0]
    into[0] = total
    for t in range(1, SUBS):
        total = total + terms[t]
        into[t] = total


def lagged_sums(terms, into, rows=ALL):
    total = jnp.zeros_like(terms[0, rows])
    for t in range(SUBS):
        into[t, rows] = total
        total = total + terms[t, rows]


def fold(x):
    return jnp.sum(x.reshape(x.shape[0] // 8, 8, x.shape[1]), axis=0)


class Sums:
    def __init__(self):
        self.held = None

    def add(self, x0, x1, x2, scale=None):
        d0, d1 = x0 - x1, x1 - x2
        terms = (d0 * x0, d0 * d0, d0 * x1 + d1 * x0, d1 * x1, d0 * d1, d1 * d1)
        terms = [fold(x) for x in terms]
        if scale is not None:
            terms = [x * scale for x in terms]
        self.held = terms if self.held is None else [a + b for a, b in zip(self.held, terms)]

    def tile(self):
        rows = [jnp.sum(x, axis=0, keepdims=True) for x in self.held]
        return jnp.concatenate(rows + [jnp.zeros((1, WIDE), F32)] * 2, axis=0)


INPUTS = (
    "b", "obs", "l0", "traj", "w_in", "w_out", "modes", "base", "scale", "limit", "ocol", "count",
    "vrow",
)
LOADS = {
    "l0": "l0", "traj": "traj", "b": "b", "modes": "fmod", "obs": "obs", "base": "base",
    "scale": "scale", "limit": "limit", "ocol": "ocol", "count": "count", "vrow": "vrow",
}
OUTPUTS = ("mult", "obs_a", "obs_b", "incr_a", "incr_b")
NAMES = (
    "shift", "vpair", "vz", "vcore", "hl", "hb", "hr", "nfw", "mret", "sret", "mful", "efw",
    "m2ret", "tfw", "qret", "m2ful", "afw", "ufw", "gat1", "gat2", "red1", "amp0", "lba", "amp1",
    "bak1", "amp2", "bak2", "red2", "clx", "nfw1", "mret1", "tfw1", "qret1", "efw1", "m2ret1",
)


def scratch_list(deep, width, hidden, total_cols):
    piece = deep // RING
    field, every = (RING, piece, width), (SUBS, piece, width)
    amps, flat = (COLN, PAD, width), (PAD, total_cols)
    coef, wide = (RING, PAD, 2 * KW), (GRPS, PAD, total_cols)
    back = (COLN, GRPS, PAD, width)
    out = {
        "fin": ((hidden, deep), F32), "fout": ((deep, hidden), F32),
        "wih": ((hidden, deep), BF16), "wil": ((hidden, deep), BF16),
        "woh": ((deep, hidden), BF16), "wol": ((deep, hidden), BF16),
        "slp": ((width, hidden), F32), "hh": ((2 * width, hidden), BF16),
        "zz": ((2 * width, deep), BF16), "ot": ((width, deep), F32),
        "vpad": ((COLN, PAD, deep), F32), "voth": ((COLN // CORES, CORES, PAD, deep), F32),
        "vah": ((GRPS, COLN * PAD, deep), BF16), "val": ((GRPS, COLN * PAD, deep), BF16),
        "seen": ((64, deep), F32), "seen2": ((64, deep), F32), "p3t": ((width, deep), F32),
        "ht": ((width, deep), F32), "qt": ((width, deep), F32),
        "cl": ((GRPS, PAD, 2 * KW), F32),
        "thi": ((total_cols, 2 * KW), BF16), "tlo": ((total_cols, 2 * KW), BF16),
        "spec": ((PAD, 2 * KW), F32), "var": ((64, 1), F32),
        "pick": ((width, 64), BF16), "pick_t": ((64, width), BF16),
        "r1": (field, F32), "p3": (field, F32), "q": (field, F32),
        "rb1": ((RING, 8, WIDE), F32), "rb2": ((COLN, 8, WIDE), F32),
    }
    for name in ("lup", "np_", "nbuf", "mup", "sb", "mfull", "ep", "ebuf", "m2up", "tp", "tbuf",
                 "qs", "m2full", "ap", "abuf", "up", "ubuf"):
        out[name] = (field, F32)
    for name in ("nt", "mt", "bt", "sbt", "l0t", "r1t", "et", "m2t", "t1t", "qst"):
        out[name] = (every, F32)
    loaded = {
        "b": (field, F32), "obs": ((64, deep), F32), "l0": (field, F32),
        "traj": ((deep, width), BF16), "fmod": ((deep // GRPS, deep), F32),
        "base": ((2 * WIDE + 2 * COLN, KW), F32), "scale": ((deep // WIDE, WIDE), F32),
        "limit": ((deep // WIDE, WIDE), jnp.int32), "ocol": ((1, 64), jnp.int32),
        "count": ((1, 1), jnp.int32), "vrow": ((1, 64), F32),
    }
    for name, kind in loaded.items():
        out["in_" + name] = kind
    for i in range(3):
        out[f"am{i}"] = (amps, F32)
        out[f"cb{i}"] = (flat, F32)
        out[f"wd{i}"] = (wide, F32)
        out[f"bk{i}"] = (back, F32)
    for i in (1, 2):
        out[f"gb{i}"] = (coef, F32)
    return out


def kernel(names, *refs):
    given = dict(zip(names, refs))
    loads = {n: (given[n], given["in_" + to]) for n, to in LOADS.items()}
    x = types.SimpleNamespace(**given)
    for n, to in LOADS.items():
        setattr(x, to, given["in_" + to])
    s, c, g = lax.axis_index("sub"), lax.axis_index("col"), lax.axis_index("grp")
    core, z = lax.rem(c, CORES), lax.div(c, CORES)
    r = s * GRPS + g
    deep, hidden, width = x.woh.shape[0], x.woh.shape[1], x.slp.shape[0]
    ring = Group(r, RING, lambda p: {"sub": lax.div(p, GRPS), "grp": lax.rem(p, GRPS)})
    subs = Group(s, SUBS, lambda p: {"sub": p})
    cols = Group(c, COLN, lambda p: {"col": p})
    pair = Group(g, GRPS, lambda p: {"grp": p})
    same = Group(z, COLN // CORES, lambda p: {"col": p * CORES + core})
    chip = Group(core, CORES, lambda p: {"col": z * CORES + p})

    def over(name, group, src, dst, all_ref):
        return Exchange(group, x.sems, NAMES.index(name), src, dst, all_ref)

    def others(ref, group):
        return ref.at[pl.ds(0, group.count - 1)]

    def next_sub(p):
        return lax.rem(lax.div(p, GRPS) + 1, SUBS)

    def forward(name, src, dst, rows=slice(0, deep // RING)):
        at = dst.at[pl.ds(0, RING - 1), rows]
        return over(name, ring, lambda p: src.at[p, rows], lambda i: dst.at[i, rows], at)

    def giving(name, src, dst, rows=slice(0, deep // RING)):
        at = dst.at[pl.ds(0, RING - 1), rows]
        return over(
            name, ring, lambda p: src.at[lax.div(p, GRPS), rows], lambda i: dst.at[i, rows], at
        )

    def giving_next(name, src, dst, rows=slice(0, deep // RING)):
        at = dst.at[pl.ds(0, RING - 1), rows]
        return over(name, ring, lambda p: src.at[next_sub(p), rows], lambda i: dst.at[i, rows], at)

    def halves(name, src, dst):
        at = others(dst, subs)
        return over(name, subs, lambda p: src.at[p * GRPS + g], lambda i: dst.at[i], at)

    def amps(name, src, dst):
        at = dst.at[:, pl.ds(0, (COLN - 1) * WIDE)]
        return over(name, cols, lambda p: src.at[p], lambda i: dst.at[:, lanes(i)], at)

    def backs(name, src, dst):
        at = others(dst, cols)
        return over(name, cols, lambda p: src.at[:, :, lanes(p)], lambda i: dst.at[i], at)

    def gathers(name, buf):
        return over(name, ring, lambda p: buf.at[r], lambda i: buf.at[i], others(buf, ring))

    def both(kind, name, src, dst):
        return [kind(n, src, dst, rows) for n, rows in zip((name, name + "1"), PARTS)]

    row = NAMES.index("shift")
    shift = pltpu.make_async_remote_copy(
        src_ref=x.l0, dst_ref=x.lup, send_sem=x.sems.at[2 * row],
        recv_sem=x.sems.at[2 * row + 1],
        device_id={"sub": lax.rem(s + SUBS - 1, SUBS)}, device_id_type=MESH,
    )
    vpair = over("vpair", pair, lambda p: x.vpad.at[c], lambda i: x.voth.at[z, core], x.voth.at[z, core])
    at = x.voth.at[pl.ds(0, same.count - 1), core]
    vz = over("vz", same, lambda p: x.voth.at[z, core], lambda i: x.voth.at[i, core], at)
    at = x.voth.at[:, 1 - core]
    vcore = over("vcore", chip, lambda p: x.voth.at[:, core], lambda i: x.voth.at[:, i], at)
    hl = halves("hl", x.l0, x.l0t)
    hb = halves("hb", x.b, x.bt)
    hr = halves("hr", x.r1, x.r1t)
    nfw = both(forward, "nfw", x.np_, x.nbuf)
    mret = both(giving_next, "mret", x.mt, x.mup)
    sret = giving("sret", x.sbt, x.sb)
    mful = giving("mful", x.mt, x.mfull)
    efw = both(forward, "efw", x.ep, x.ebuf)
    m2ret = both(giving_next, "m2ret", x.m2t, x.m2up)
    tfw = both(forward, "tfw", x.tp, x.tbuf)
    qret = both(giving, "qret", x.qst, x.qs)
    m2ful = giving("m2ful", x.m2t, x.m2full)
    afw = forward("afw", x.ap, x.abuf)
    ufw = forward("ufw", x.up, x.ubuf)
    gat1, gat2 = gathers("gat1", x.gb1), gathers("gat2", x.gb2)
    red1 = gathers("red1", x.rb1)
    red2 = over("red2", cols, lambda p: x.rb2.at[c], lambda i: x.rb2.at[i], others(x.rb2, cols))
    amp0, amp1, amp2 = (amps(f"amp{i}", getattr(x, f"am{i}"), getattr(x, f"cb{i}")) for i in range(3))
    lba, bak1, bak2 = (
        backs(n, getattr(x, f"wd{i}"), getattr(x, f"bk{i}"))
        for i, n in enumerate(("lba", "bak1", "bak2"))
    )
    clx = over("clx", pair, lambda p: x.cl.at[g], lambda i: x.cl.at[i], x.cl.at[1 - g])
    sent = [vpair, vz, vcore, hl, hb, hr, *nfw, *mret, sret, mful, *efw, *m2ret, *tfw, *qret,
            m2ful, afw, ufw, gat1, gat2, red1, red2, amp0, amp1, amp2, lba, bak1, bak2, clx]

    strips = deep // STRIP

    def get_in(j):
        return pltpu.make_async_copy(x.w_in.at[chunk(j), :], x.fin.at[chunk(j), :], x.local.at[j])

    def get_out(j):
        at = chunk(j, STRIP)
        return pltpu.make_async_copy(x.w_out.at[at, :], x.fout.at[at, :], x.local.at[hidden // CHUNK + j])

    load = {
        n: pltpu.make_async_copy(*loads[n], x.local.at[hidden // CHUNK + strips + i]) for i, n in enumerate(loads)
    }
    for n in ("l0", "traj", "b"):
        load[n].start()
    for j in range(hidden // CHUNK):
        get_in(j).start()
    for j in range(strips):
        get_out(j).start()
    for n in tuple(load)[3:]:
        load[n].start()

    def first_half(columns):
        weights = (x.woh, x.wol) if columns else (x.wih, x.wil)

        def step(j, carry):
            at = (slice(None), chunk(j)) if columns else (chunk(j), slice(None))
            pair_ = (weights[0][at], weights[1][at])
            value = mm3s(x.zz[...], pair_, ROWS if columns else BACK)
            x.hh[:, chunk(j)] = stack(value * x.slp[:, chunk(j)])
            return carry

        lax.fori_loop(0, hidden // CHUNK, step, 0)

    def second_half(columns):
        weights = (x.wih, x.wil) if columns else (x.woh, x.wol)

        def part(at):
            where = (slice(None), at) if columns else (at, slice(None))
            pair_ = (weights[0][where], weights[1][where])
            x.ot[:, at] = mm3s(x.hh[...], pair_, ROWS if columns else BACK)

        def step(j, carry):
            part(chunk(j))
            return carry

        lax.fori_loop(0, deep // CHUNK, step, 0)
        left = deep % CHUNK
        if left:
            part(pl.ds(deep - left, left))

    def adjoint(zt):
        x.zz[...] = stack(zt)
        first_half(True)
        second_half(True)
        return x.ot[...]

    def tangent(zt, between=lambda: None):
        x.zz[...] = stack(zt)
        first_half(False)
        between()
        second_half(False)
        return x.ot[...]

    def whole(ref):
        return ref[...].reshape(deep, width)

    def put(ref, value_t):
        ref[...] = value_t.T.reshape(ref.shape)

    def amplitudes(ref, into):
        high, low = split(whole(ref))
        value = mm(x.vah[g], jnp.concatenate([high, low], axis=1), ROWS)
        value = value[:, :width] + value[:, width:] + mm(x.val[g], high, ROWS)
        into[...] = value.reshape(into.shape)

    def restored_t(bk):
        total = None
        for h in range(GRPS):
            turned = stack(bk[:, h].reshape(COLN * PAD, width).T)
            term = mm3s(turned, (x.vah[h], x.val[h]), ROWS)
            total = term if total is None else total + term
        return total

    def coefficients(cb):
        return mm3(split(cb[...]), (x.thi[...], x.tlo[...]), ROWS) * x.spec[...]

    def spread_back(values, into):
        value = mm3s(stack(values), (x.thi[...], x.tlo[...]), BACK)
        into[...] = value.reshape(into.shape)

    def summed(gb):
        parts = []
        for h in range(GRPS):
            total = gb[GRPS * (SUBS - 1) + h]
            for u in range(SUBS - 1):
                total = total + jnp.where(u + 1 <= s, 1.0, 0.0) * gb[GRPS * u + h]
            parts.append(total)
        return jnp.concatenate(parts, axis=0)

    def pick_rows(vt):
        high, low = split(vt)
        return mm(x.pick_t[...], high, ROWS) + mm(x.pick_t[...], low, ROWS)

    def spread_rows(values):
        high, low = split(values)
        return mm(x.pick[...], high, ROWS) + mm(x.pick[...], low, ROWS)

    has_later = jnp.where(s < SUBS - 1, 1.0, 0.0)
    leads = jnp.where(g == 0, 1.0, 0.0)

    owned = x.fmod.shape[0] // COLN
    meet(ring, cols)
    load["l0"].wait()
    load["traj"].wait()
    traj_t = x.traj[...].astype(F32).T
    x.zz[:width] = traj_t.astype(BF16)
    met(ring, cols)
    shift.start()
    load["b"].wait()
    hb.start()
    x.bt[s] = x.b[r]
    x.l0t[s] = x.l0[r]

    def open_in(j, carry):
        get_in(j).wait()
        high, low = split(x.fin[chunk(j), :])
        x.wih[chunk(j), :] = high
        x.wil[chunk(j), :] = low
        inner = mm(x.zz[:width], high, BACK) + mm(x.zz[:width], low, BACK)
        x.slp[:, chunk(j)] = 1.0 - jnp.tanh(inner) ** 2
        return carry

    lax.fori_loop(0, hidden // CHUNK, open_in, 0)

    def open_out(j, carry):
        get_out(j).wait()
        at = chunk(j, STRIP)
        high, low = split(x.fout[at, :])
        x.woh[at, :] = high
        x.wol[at, :] = low
        return carry

    lax.fori_loop(0, strips, open_out, 0)
    shift.wait_recv()
    put(x.np_, adjoint(whole(x.lup).T) * has_later)
    for part in nfw:
        part.start()
    x.nbuf[r] = x.np_[r]
    for n in tuple(load)[3:]:
        load[n].wait()
    for i in range(COLN):
        x.vpad[i, :owned] = x.fmod[i * owned:(i + 1) * owned]
        x.vpad[i, owned:] = jnp.zeros((PAD - owned, deep), F32)
    vpair.start()
    high, low = split(x.vpad[...].reshape(COLN * PAD, deep))
    x.vah[g] = high
    x.val[g] = low
    amplitudes(x.l0, x.am0)
    amp0.start()
    x.cb0[:, lanes(c)] = x.am0[c]

    def iota(shape, dim):
        return lax.broadcasted_iota(jnp.int32, shape, dim)

    total_cols = width * COLN
    first_mode = g * (owned * COLN) + c * owned
    scales = limits = jnp.zeros((PAD, WIDE), F32)
    for q in range(deep // WIDE):
        own = iota((PAD, WIDE), 1) + q * WIDE == iota((PAD, WIDE), 0) + first_mode
        scales = scales + jnp.where(own, x.scale[q:q + 1, :], 0.0)
        limits = limits + jnp.where(own, x.limit[q:q + 1, :].astype(F32), 0.0)
    scales = jnp.sum(scales, axis=1, keepdims=True)
    limits = jnp.sum(limits, axis=1, keepdims=True)
    wave = iota((PAD, KW), 1).astype(F32)
    decay = jnp.exp(-0.5 * (2.0 * math.pi * wave * scales / total_cols) ** 2)
    factor = jnp.where(iota((PAD, KW), 1) == 0, 1.0, 2.0) / total_cols
    values = decay * factor * jnp.where(wave < limits, 1.0, 0.0)
    x.spec[:, :KW] = values
    x.spec[:, KW:] = values
    slots = x.obs.shape[0]
    chosen = jnp.where(iota((1, slots), 1) < x.count[...], x.ocol[...] - c * width, -1)
    chosen = chosen.astype(F32)
    eye = iota((slots, slots), 0) == iota((slots, slots), 1)
    down = jnp.sum(jnp.where(eye, chosen, 0.0), axis=1, keepdims=True)
    x.var[...] = jnp.sum(jnp.where(eye, x.vrow[...], 0.0), axis=1, keepdims=True)
    near = iota((width, slots), 0).astype(F32) == chosen
    x.pick[...] = jnp.where(near, 1.0, 0.0).astype(BF16)
    near = iota((slots, width), 1).astype(F32) == down
    x.pick_t[...] = jnp.where(near, 1.0, 0.0).astype(BF16)

    def open_table(p, carry):
        cos_in, sin_in = x.base[:WIDE], x.base[WIDE:2 * WIDE]
        cos_at = x.base[pl.ds(2 * WIDE + p, 1)]
        sin_at = x.base[pl.ds(2 * WIDE + COLN + p, 1)]
        rows = chunk(p, WIDE)
        high, low = split(cos_at * cos_in - sin_at * sin_in)
        x.thi[rows, :KW], x.tlo[rows, :KW] = high, low
        high, low = split(sin_at * cos_in + cos_at * sin_in)
        x.thi[rows, KW:], x.tlo[rows, KW:] = high, low
        return carry

    lax.fori_loop(0, COLN, open_table, 0)
    vpair.wait_recv()
    vz.start()
    x.ht[...] = spread_rows(x.obs[...] / x.var[...])
    for rows, come, go in zip(PARTS, nfw, mret):
        come.wait_recv()
        pair_sums(x.nbuf, x.nt, rows)
        suffix_sums(x.nt, x.mt, rows)
        go.start()
    x.mup[r] = x.mt[lax.rem(s + 1, SUBS)]
    hb.wait_recv()
    prefix_sums(x.bt, x.sbt)
    sret.start()
    x.sb[r] = x.sbt[s]
    mful.start()
    x.mfull[r] = x.mt[s]
    amp0.wait_recv()
    x.cl[g] = coefficients(x.cb0)
    for part in mret:
        part.wait_recv()
    amplitudes(x.mup, x.am1)
    amp1.start()
    clx.start()
    x.cb1[:, lanes(c)] = x.am1[c]
    vz.wait_recv()
    vcore.start()
    put(x.ep, adjoint((whole(x.mup) - whole(x.lup)).T) * has_later - leads * x.ht[...])
    amp1.wait_recv()
    x.gb1[r] = coefficients(x.cb1)
    gat1.start()
    for part in efw:
        part.start()
    x.ebuf[r] = x.ep[r]
    clx.wait_recv()
    spread_back(x.cl[...].reshape(GRPS * PAD, 2 * KW), x.wd0)
    vcore.wait_recv()
    high, low = split(x.voth[...].reshape(COLN * PAD, deep))
    x.vah[1 - g] = high
    x.val[1 - g] = low
    gat1.wait_recv()
    spread_back(summed(x.gb1), x.wd1)
    bak1.start()
    x.bk1[c] = x.wd1[:, :, lanes(c)]
    for rows, come, go in zip(PARTS, efw, m2ret):
        come.wait_recv()
        pair_sums(x.ebuf, x.et, rows)
        suffix_sums(x.et, x.m2t, rows)
        go.start()
    m2ful.start()
    x.m2full[r] = x.m2t[s]
    x.m2up[r] = x.m2t[lax.rem(s + 1, SUBS)]
    for part in m2ret:
        part.wait_recv()
    amplitudes(x.m2up, x.am2)
    amp2.start()
    lba.start()
    x.cb2[:, lanes(c)] = x.am2[c]
    x.bk0[c] = x.wd0[:, :, lanes(c)]
    sret.wait_recv()
    bak1.wait_recv()
    p3t = whole(x.sb).T - restored_t(x.bk1)
    x.p3t[...] = p3t

    def between():
        amp2.wait_recv()
        x.gb2[r] = coefficients(x.cb2)
        gat2.start()

    put(x.tp, tangent(p3t, between))
    for part in tfw:
        part.start()
    x.tbuf[r] = x.tp[r]
    gat2.wait_recv()
    spread_back(summed(x.gb2), x.wd2)
    bak2.start()
    x.bk2[c] = x.wd2[:, :, lanes(c)]
    put(x.p3, x.p3t[...])
    x.seen[...] = pick_rows(x.p3t[...])
    for rows, come, go in zip(PARTS, tfw, qret):
        come.wait_recv()
        pair_sums(x.tbuf, x.t1t, rows)
        lagged_sums(x.t1t, x.qst, rows)
        go.start()
    x.qs[r] = x.qst[s]
    a2 = adjoint(whole(x.m2up).T) * has_later
    put(x.ap, a2 + leads * spread_rows(x.seen[...] / x.var[...]))
    afw.start()
    x.abuf[r] = x.ap[r]
    lba.wait_recv()
    x.r1[...] = x.b[...] - restored_t(x.bk0).T.reshape(x.r1.shape)
    hr.start()
    hl.start()
    x.r1t[s] = x.r1[r]
    for part in qret:
        part.wait_recv()
    bak2.wait_recv()
    qt = whole(x.qs).T - restored_t(x.bk2)
    x.qt[...] = qt
    put(x.up, tangent(qt))
    ufw.start()
    x.ubuf[r] = x.up[r]
    put(x.q, x.qt[...])
    x.seen2[...] = pick_rows(x.qt[...])
    sums = Sums()
    for i in range(deep // WIDE):
        at = slice(i * WIDE, (i + 1) * WIDE)
        sums.add(x.obs[:, at], -x.seen[:, at], -x.seen2[:, at], leads)
    hl.wait_recv()
    afw.wait_recv()
    blank = jnp.zeros_like(x.mt[0])
    for t in range(SUBS):
        here = x.mt[t] - x.l0t[t]
        later = x.mt[t + 1] - x.l0t[t + 1] if t < SUBS - 1 else blank
        sums.add(here - later, x.et[t], x.abuf[2 * t] + x.abuf[2 * t + 1])
    hr.wait_recv()
    ufw.wait_recv()
    for t in range(SUBS):
        x1 = x.t1t[t - 1] if t else blank
        x2 = x.ubuf[2 * t - 2] + x.ubuf[2 * t - 1] if t else blank
        sums.add(x.r1t[t], x1, x2)
    x.rb1[r] = sums.tile()
    red1.start()
    red1.wait_recv()
    total = x.rb1[0]
    for i in range(1, RING):
        total = total + x.rb1[i]
    x.rb2[c] = total
    red2.start()
    mful.wait_recv()
    m2ful.wait_recv()
    red2.wait_recv()
    total = x.rb2[0]
    for i in range(1, COLN):
        total = total + x.rb2[i]
    gram = jnp.sum(total, axis=1, keepdims=True)
    gram = [gram[i:i + 1] for i in range(6)]
    a = gram[0] / gram[1]
    b = 1.0 - a
    upper = b * b * gram[0] + a * b * gram[2] + a * a * gram[3]
    lower = b * b * gram[1] + 2.0 * a * b * gram[4] + a * a * gram[5]
    a_next = upper / lower
    one, two = a + a_next * b, a_next * a
    move = whole(x.mfull) - whole(x.l0)
    x.mult[...] = (one * move + two * whole(x.m2full)).reshape(x.mult.shape)
    x.incr_a[...] = (one * whole(x.p3)).reshape(x.incr_a.shape)
    x.incr_b[...] = (two * whole(x.q)).reshape(x.incr_b.shape)
    x.obs_a[...] = one * (x.obs[...] / x.var[...])
    x.obs_b[...] = two * (x.seen[...] / x.var[...])
    for one in sent:
        one.wait_send()
    shift.wait_send()


def on_device(
    first_rhs,
    innovations,
    start_mult,
    trajectory,
    weight_in,
    weight_out,
    vertical_modes,
    length_scale,
    band_limit,
    obs_col,
    obs_count,
    obs_var,
):
    deep, width = first_rhs.shape[1:]
    slots = innovations.shape[1]
    hidden = weight_in.shape[0]
    total_cols = width * COLN
    field = (RING, deep // RING, width)

    vmem = pl.BlockSpec(memory_space=pltpu.VMEM)
    away = pl.BlockSpec(memory_space=pl.ANY)
    args = dict(
        b=first_rhs.reshape(field), obs=innovations[0], l0=start_mult.reshape(field),
        traj=trajectory[0], w_in=weight_in, w_out=weight_out, modes=vertical_modes,
        base=jnp.asarray(base_tables(total_cols)), scale=length_scale.reshape(-1, WIDE),
        limit=band_limit.reshape(-1, WIDE), ocol=obs_col, count=obs_count, vrow=obs_var,
    )
    scratch = scratch_list(deep, width, hidden, total_cols)
    names = INPUTS + OUTPUTS + tuple(scratch) + ("local", "sems")
    shapes = (field, (slots, deep), (slots, deep), field, field)
    move, obs_a, obs_b, incr_a, incr_b = pl.pallas_call(
        lambda *refs: kernel(names, *refs),
        name="saddle",
        out_shape=[pltpu.VMEM(shape, F32) for shape in shapes],
        in_specs=[away] * len(INPUTS),
        out_specs=[vmem] * len(shapes),
        scratch_shapes=[pltpu.VMEM(*scratch[n]) for n in scratch]
        + [
            pltpu.SemaphoreType.DMA((hidden // CHUNK + deep // STRIP + len(LOADS),)),
            pltpu.SemaphoreType.DMA((2 * len(NAMES),)),
        ],
        compiler_params=pltpu.CompilerParams(collective_id=0, has_side_effects=True, vmem_limit_bytes=59_000_000),
    )(*(args[n] for n in INPUTS))
    mult = start_mult + move.reshape(1, deep, width)
    incr = incr_a + incr_b
    return mult, (obs_a - obs_b)[None], incr.reshape(1, deep, width)


def solution(mesh):
    in_specs = (
        P("sub", None, "col"),
        P("sub", "col", None),
        P("sub", None, "col"),
        P("sub", None, "col"),
        P("grp", None),
        P(None, "grp"),
        P("grp", None),
        P(),
        P(),
        P("sub", "col"),
        P("sub", "col"),
        P("sub", "col"),
    )
    out_specs = (P("sub", None, "col"), P("sub", "col", None), P("sub", None, "col"))
    return jax.shard_map(
        on_device, mesh=mesh, in_specs=in_specs, out_specs=out_specs, check_vma=False
    )
```
